32 devices in a mesh: lb: 2 (over y), rb: 4 (over z), wa: 4 (over x, core).
Axes of the slice: x: 2, y: 2, z: 4, core: 2. Of those that a mesh axis runs over, the one named last changes fastest.
Arguments:
- state: bfloat16 [4, 4, 4, 1024, 1024], P('wa', None, None, 'lb', 'rb'), may hold values from -14 to 14
- left_env: bfloat16 [3, 4, 1024, 4, 1024], P(None, None, 'lb', 'wa'), may hold values from -1 to 2.5
- right_env: bfloat16 [3, 4, 1024, 4, 1024], P(None, None, 'rb', 'wa'), may hold values from -1 to 2.5
- site_one: float32 [3, 3, 2, 2], replicated, may hold values from -2 to 3
- site_two: float32 [3, 3, 2, 2], replicated, may hold values from -2 to 3
Outputs:
- next_vector: float32 [4, 4, 4, 1024, 1024], P('wa', None, None, 'lb', 'rb')
- coefficients: float32 [2], replicated
The draws below stay inside these ranges and needn't reach their ends.
All inputs are finite; a program needn't handle non-finite values.
Results may differ from the reference program's by a relative error of at most 0.02.
Values may be sent and summed in bfloat16 or wider, within the bound.
A program may use at most 192 MiB of HBM per device.

```python
import math
import jax
import jax.numpy as jnp
from jax import lax

BOND = 4096
BLOCKS = 4
BLOCK_ROWS = 1024
DW = 3
SITE_DIM = 2
PHYS = 4
LEFT_RANGES = 2
RIGHT_RANGES = 4


def environment(key):
    noise_key, diagonal_key = jax.random.split(key)
    full_shape = (DW, BLOCKS, BLOCK_ROWS, BLOCKS, BLOCK_ROWS)
    noise_values = jnp.clip(jax.random.normal(noise_key, full_shape, jnp.float32), -4.0, 4.0)
    diagonal = jax.random.uniform(diagonal_key, (DW, BLOCKS, BLOCK_ROWS), jnp.float32, 0.5, 1.5)
    block_identity = (lax.broadcasted_iota(jnp.int32, (BLOCKS, BLOCKS), 0) == lax.broadcasted_iota(jnp.int32, (BLOCKS, BLOCKS), 1)).astype(jnp.float32)
    row_identity = (lax.broadcasted_iota(jnp.int32, (BLOCK_ROWS, BLOCK_ROWS), 0) == lax.broadcasted_iota(jnp.int32, (BLOCK_ROWS, BLOCK_ROWS), 1)).astype(jnp.float32)
    identity = block_identity[:, None, :, None] * row_identity[None, :, None, :]
    values = noise_values / math.sqrt(BOND) + diagonal[:, :, :, None, None] * identity[None]
    return values.astype(jnp.bfloat16)


def draw_left_env(key, part):
    return environment(jax.random.fold_in(key, 11))


def draw_right_env(key, part):
    return environment(jax.random.fold_in(key, 23))


def site_tensor(key):
    full_shape = (DW, DW, SITE_DIM, SITE_DIM)
    noise_values = jnp.clip(jax.random.normal(key, full_shape, jnp.float32), -4.0, 4.0)
    bond_identity = (lax.broadcasted_iota(jnp.int32, (DW, DW), 0) == lax.broadcasted_iota(jnp.int32, (DW, DW), 1)).astype(jnp.float32)
    spin_identity = (lax.broadcasted_iota(jnp.int32, (SITE_DIM, SITE_DIM), 0) == lax.broadcasted_iota(jnp.int32, (SITE_DIM, SITE_DIM), 1)).astype(jnp.float32)
    return bond_identity[:, :, None, None] * spin_identity[None, None] + 0.5 * noise_values


def draw_site_one(key, part):
    return site_tensor(jax.random.fold_in(key, 41))


def draw_site_two(key, part):
    return site_tensor(jax.random.fold_in(key, 53))


def draw_state(key, part):
    noise_key = jax.random.fold_in(key, 37)
    full_shape = (BLOCKS, BLOCKS, PHYS, BLOCK_ROWS, BLOCK_ROWS)
    left_pos = lax.broadcasted_iota(jnp.float32, (BLOCK_ROWS, BLOCK_ROWS), 0) / BLOCK_ROWS
    rising = jnp.exp(math.log(3.3) * left_pos)
    noise_values = jnp.clip(jax.random.normal(noise_key, full_shape, jnp.float32), -4.0, 4.0)
    scaled = noise_values * rising[None, None, None]
    return scaled.astype(jnp.bfloat16)


def setup_inputs(seed: int = 0) -> dict:
    seeds = jax.random.split(jax.random.key(seed), 6)
    state = draw_state(jax.random.fold_in(seeds[5], 71), 0)
    left_env = draw_left_env(jax.random.fold_in(seeds[5], 71), 0)
    right_env = draw_right_env(jax.random.fold_in(seeds[5], 71), 0)
    site_one = draw_site_one(jax.random.fold_in(seeds[5], 71), 0)
    site_two = draw_site_two(jax.random.fold_in(seeds[5], 71), 0)
    return {"state": state, "left_env": left_env, "right_env": right_env, "site_one": site_one, "site_two": site_two}


EPSILON = 1e-06

def pair_tensor(site_one, site_two):
    joined = jnp.einsum('wuac,uvbd->wvabcd', site_one.astype(jnp.float32), site_two.astype(jnp.float32), precision=lax.Precision.HIGHEST)
    mpo_width = site_one.shape[0]
    states = site_one.shape[2] * site_two.shape[2]
    return joined.reshape(mpo_width, mpo_width, states, states)

def reference(state, left_env, right_env, site_one, site_two):
    mpo_pair = pair_tensor(site_one, site_two)
    mpo_width = left_env.shape[0]
    left_rows = BLOCK_ROWS // LEFT_RANGES
    right_rows = BLOCK_ROWS // RIGHT_RANGES
    trailing = BLOCKS * PHYS * BLOCK_ROWS
    state_rows = jnp.transpose(state, (0, 3, 1, 2, 4))

    def left_contract(env_slice):

        def add_range(running, position):
            offset = (position * left_rows).astype(jnp.int32)
            env_rows = lax.dynamic_slice_in_dim(env_slice, offset, left_rows, 1).reshape(BLOCKS * left_rows, BLOCKS * BLOCK_ROWS)
            state_part = lax.dynamic_slice_in_dim(state_rows, offset, left_rows, 1).reshape(BLOCKS * left_rows, trailing)
            partial_value = jnp.dot(env_rows.T, state_part, preferred_element_type=jnp.float32)
            rounded = lax.optimization_barrier(partial_value.astype(jnp.bfloat16)).astype(jnp.float32)
            return (running + rounded, None)
        running, _ = lax.scan(add_range, jnp.zeros((BLOCKS * BLOCK_ROWS, trailing), jnp.float32), jnp.arange(LEFT_RANGES, dtype=jnp.int32))
        return running
    left_sum = lax.map(left_contract, left_env)
    left_sum = left_sum.reshape(mpo_width, BLOCKS * BLOCK_ROWS, BLOCKS, PHYS, BLOCK_ROWS)
    mixed_state = jnp.einsum('wphsn,wvst->ptvhn', left_sum, mpo_pair, precision=lax.Precision.HIGHEST).astype(jnp.bfloat16)
    env_right = right_env.reshape(mpo_width, BLOCKS, BLOCK_ROWS, BLOCKS * BLOCK_ROWS)

    def add_right(running, position):
        offset = (position * right_rows).astype(jnp.int32)
        mixed_part = lax.dynamic_slice_in_dim(mixed_state, offset, right_rows, 4).reshape(BLOCKS * BLOCK_ROWS * PHYS, mpo_width * BLOCKS * right_rows)
        env_part = lax.dynamic_slice_in_dim(env_right, offset, right_rows, 2).reshape(mpo_width * BLOCKS * right_rows, BLOCKS * BLOCK_ROWS)
        partial_value = jnp.dot(mixed_part, env_part, preferred_element_type=jnp.float32)
        rounded = lax.optimization_barrier(partial_value.astype(jnp.bfloat16)).astype(jnp.float32)
        return (running + rounded, None)
    image_rows, _ = lax.scan(add_right, jnp.zeros((BLOCKS * BLOCK_ROWS * PHYS, BLOCKS * BLOCK_ROWS), jnp.float32), jnp.arange(RIGHT_RANGES, dtype=jnp.int32))
    applied = jnp.transpose(image_rows.reshape(BLOCKS, BLOCK_ROWS, PHYS, BLOCKS, BLOCK_ROWS), (0, 3, 2, 1, 4))
    state_values = state.astype(jnp.float32)
    norm_sq = jnp.mean(state_values * state_values) + EPSILON
    projection = jnp.mean(state_values * applied)
    alpha_coef = projection / norm_sq
    residual = (applied - alpha_coef * state_values) / jnp.sqrt(norm_sq)
    beta_coef = jnp.sqrt(jnp.mean(residual * residual) + EPSILON)
    return (residual / beta_coef, jnp.stack([alpha_coef, beta_coef]))
```

```python
import functools
import jax
import jax.numpy as jnp
from jax import lax
from jax.experimental import pallas as pl
from jax.experimental.pallas import tpu as pltpu
from jax.sharding import PartitionSpec as P

EPSILON = 1e-06
CHUNKS = 4
GATHERS = 2


def pair_tensor(site_one, site_two):
    joined = jnp.einsum("wuac,uvbd->wvabcd", site_one, site_two, precision=lax.Precision.HIGHEST)
    mpo_width = site_one.shape[0]
    states = site_one.shape[2] * site_two.shape[2]
    return joined.reshape(mpo_width, mpo_width, states, states)


def mix_kernel(terms, pair_ref, *refs):
    out_ref = refs[terms]
    width, _, states, rows, _ = refs[0].shape
    step = 16

    @pl.loop(0, rows // step)
    def _(block):
        span = pl.ds(pl.multiple_of(block * step, step), step)
        planes = []
        for w in range(width):
            for s in range(states):
                value = refs[0][w, 0, s, span, :].astype(jnp.float32)
                for other in refs[1:terms]:
                    value = value + other[w, 0, s, span, :].astype(jnp.float32)
                planes.append(value)
        for v in range(width):
            for t in range(states):
                total = None
                for w in range(width):
                    for s in range(states):
                        entry = pair_ref[((w * width + v) * states + s) * states + t]
                        term = planes[w * states + s] * entry
                        total = term if total is None else total + term
                out_ref[v, 0, t, span, :] = total.astype(out_ref.dtype)


def mix(pair, parts):
    width, blocks, states, rows, lanes = parts[0].shape
    spec = pl.BlockSpec((width, 1, states, rows, lanes), lambda h: (0, h, 0, 0, 0))
    count = width * states
    size = parts[0].size
    return pl.pallas_call(
        functools.partial(mix_kernel, len(parts)),
        grid=(blocks,),
        out_shape=jax.ShapeDtypeStruct(parts[0].shape, jnp.bfloat16),
        in_specs=[pl.BlockSpec(memory_space=pltpu.SMEM)] + [spec] * len(parts),
        out_specs=spec,
        cost_estimate=pl.CostEstimate(
            flops=2 * size * count * 16, bytes_accessed=2 * size * (len(parts) + 1), transcendentals=0
        ),
    )(pair.reshape(-1), *parts)


def body(state, left_env, right_env, site_one, site_two):
    pair = pair_tensor(site_one, site_two)
    lefts, rights, owners = (lax.axis_size(name) for name in ("lb", "rb", "wa"))
    mine = lax.axis_index("lb")
    here = lax.axis_index("wa")
    _, blocks, _, _, _ = state.shape
    entries = float(state.size * lefts * rights * owners)

    group = blocks // GATHERS
    gathered = []
    for h in range(0, blocks, group):
        gathered.append(lax.all_gather(state[:, h : h + group], "wa", axis=0, tiled=True))
    turned = jnp.transpose(left_env[:, :, :, 0, :], (0, 1, 3, 2))
    owned = turned.shape[2] // lefts
    chunk = owned // CHUNKS

    def left_part(owner, position):
        rows = lax.dynamic_slice_in_dim(turned, owner * owned + position * chunk, chunk, 2)
        return [
            jnp.einsum(
                "wgpm,ghsmn->whspn", rows, part, preferred_element_type=jnp.float32
            ).astype(jnp.bfloat16)
            for part in gathered
        ]

    envs = {0: right_env[:, :, :, 0, :]}
    bit = owners // 2
    while bit:
        swap = [(a, a ^ bit) for a in range(owners)]
        for r in list(envs):
            envs[r ^ bit] = lax.ppermute(envs[r], "wa", swap)
        bit //= 2
    order = sorted(envs)
    near, far = order[: owners // 2], order[owners // 2 :]
    width, wide = envs[0].shape[0], envs[0].shape[3]

    def joined(pack):
        env = jnp.concatenate([envs[r] for r in pack], axis=3)
        return env.reshape(width, blocks, -1, len(pack), wide)

    packs = [(pack, joined(pack)) for pack in (near, far, order)]

    images = {r: [] for r in order}
    for position in range(CHUNKS):
        arrived = []
        for shift in range(1, lefts):
            sent = left_part(lax.rem(mine + shift, lefts), position)
            ring = [(a, (a + shift) % lefts) for a in range(lefts)]
            arrived.append([lax.ppermute(piece, "lb", ring) for piece in sent])
        parts = [jnp.concatenate(p, axis=1) for p in [left_part(mine, position)] + arrived]
        mixed = mix(pair, parts)
        for pack, env in packs[:2] if position == 0 else packs[2:]:
            part = jnp.einsum("vhtpn,vhndq->dtpq", mixed, env, preferred_element_type=jnp.float32).astype(jnp.bfloat16)
            part = lax.psum_scatter(part, "rb", scatter_dimension=3, tiled=True)
            for r, piece in zip(pack, part):
                images[r].append(piece)
    applied = [jnp.concatenate(images[r], axis=1).astype(jnp.float32) for r in order]
    vectors = [
        lax.dynamic_index_in_dim(state[0], here ^ r, 0, keepdims=False).astype(jnp.float32)
        for r in order
    ]
    state_values = state.astype(jnp.float32)
    terms = jnp.stack(
        [
            jnp.sum(state_values * state_values),
            sum(jnp.sum(s * a) for s, a in zip(vectors, applied)),
            sum(jnp.sum(a * a) for a in applied),
        ]
    )
    for name in ("wa", "lb", "rb"):
        size, bit = lax.axis_size(name), 1
        while bit < size:
            terms = terms + lax.ppermute(terms, name, [(a, a ^ bit) for a in range(size)])
            bit *= 2
    squares, crossed, image_squares = terms
    norm_sq = squares / entries + EPSILON
    projection = crossed / entries
    alpha_coef = projection / norm_sq
    beta_coef = jnp.sqrt((image_squares / entries - alpha_coef * projection) / norm_sq + EPSILON)
    scale = 1.0 / (jnp.sqrt(norm_sq) * beta_coef)
    result = jnp.zeros(state.shape, jnp.float32)
    for r, s, a in zip(order, vectors, applied):
        value = (a - alpha_coef * s) * scale
        result = lax.dynamic_update_slice(result, value[None, None], (0, here ^ r, 0, 0, 0))
    return (result, jnp.stack([alpha_coef, beta_coef]))


MESH = pl.DeviceIdType.MESH
STEP = 32
DEPTH = 8
HOP = 2


def line_kernel(
    sizes,
    pair_ref,
    own_ref,
    near_ref,
    far_ref,
    env_ref,
    right_ref,
    out_ref,
    psi,
    images,
    mixed,
    rows_buf,
    parts,
    arrived,
    sums,
    from_low,
    from_high,
    done,
    load_sem,
    psi_send,
    psi_recv,
    right_load,
    right_send,
    right_recv,
    rows_sem,
    part_send,
    part_recv,
    sum_send,
    low_recv,
    high_recv,
    low_free,
    high_free,
    done_sem,
):
    width, blocks, states, depth, line = sizes
    chunks = env_ref.shape[0]
    units = 4 * chunks
    early = chunks // 4
    pairs = blocks * states
    mine = lax.axis_index("lb")
    place = lax.axis_index("rb")
    here = lax.axis_index("wa")
    beside = here + 1 - 2 * lax.rem(here, 2)
    across = lax.rem(here + 2, 4)
    corner = 3 - here
    partner = (mine, place, beside)
    opposite = (mine, place, across)
    other = (1 - mine, place, here)
    higher = (mine, lax.rem(place + 1, line), here)
    lower = (mine, lax.rem(place + line - 1, line), here)

    local = []
    for n, (source, owner) in enumerate(((own_ref, here), (near_ref, beside), (far_ref, across))):
        span = pl.ds(pl.multiple_of(owner * depth, depth), depth)
        local.append(pltpu.make_async_copy(source, psi.at[:, span, :], load_sem.at[n]))
    lanes = right_ref.shape[1] // line
    half = lanes // 2
    for part in range(2):
        for d in range(line):
            local.append(
                pltpu.make_async_copy(
                    right_ref.at[:, pl.ds(d * lanes + part * half, half)],
                    images.at[part, :, pl.ds(d * half, half)],
                    right_load.at[part, d],
                )
            )
    for copy in local:
        copy.start()

    barrier = pltpu.get_barrier_semaphore()
    for device in (partner, opposite, other, higher, lower):
        pl.semaphore_signal(barrier, inc=1, device_id=device, device_id_type=MESH)
    pl.semaphore_wait(barrier, 5)

    def remote(source, target, send, recv, device):
        return pltpu.make_async_remote_copy(
            src_ref=source, dst_ref=target, send_sem=send, recv_sem=recv, device_id=device, device_id_type=MESH
        )

    span = pl.ds(pl.multiple_of(across * depth, depth), depth)
    relay = remote(far_ref, psi.at[:, span, :], psi_send.at[0], psi_recv.at[0], partner)
    relay.start()

    def rows_copy(c):
        slot = lax.rem(c, 2)
        return pltpu.make_async_copy(env_ref.at[c], rows_buf.at[slot], rows_sem.at[slot])

    rows_copy(0).start()
    for copy in local:
        copy.wait()

    def image_copy(n, source, target, device):
        return remote(images.at[source], images.at[target], right_send.at[n], right_recv.at[n], device)

    beside_copies = [image_copy(0, 0, 2, partner), image_copy(1, 1, 3, partner)]
    across_copies = [image_copy(2, 0, 4, opposite), image_copy(3, 1, 6, opposite)]
    corner_copies = [image_copy(4, 4, 5, partner), image_copy(5, 6, 7, partner)]
    for copy in across_copies + beside_copies:
        copy.start()
    relay.wait()

    def part_copy(c):
        slot = lax.rem(c, 2)
        target = lax.rem(c, 4)
        return remote(
            parts.at[slot, 1 - mine], arrived.at[target], part_send.at[slot], part_recv.at[target], other
        )

    def left(c):
        slot = lax.rem(c, 2)

        @pl.when(c >= 2)
        def _():
            part_copy(c - 2).wait_send()

        rows_copy(c).wait()

        @pl.when(c + 1 < chunks)
        def _():
            rows_copy(c + 1).start()

        def one(p, carry):
            value = jnp.dot(rows_buf[slot], psi[p], preferred_element_type=jnp.float32)
            value = value.astype(jnp.bfloat16)
            rows = value.shape[0] // 2
            parts[slot, 0, p] = value[:rows]
            parts[slot, 1, p] = value[rows:]
            return carry

        lax.fori_loop(0, pairs, one, 0)
        part_copy(c).start()

    def front(c):
        @pl.when(c + 1 < chunks)
        def _():
            left(c + 1)

        part_copy(c).wait_recv()
        slot = lax.rem(c, 2)
        source = lax.rem(c, 4)
        target = lax.rem(c, DEPTH)
        tile = 16
        wide = psi.shape[2]

        def one(h, carry):
            for step in range(STEP // tile):
                planes = []
                for w in range(width):
                    for s in range(states):
                        span = pl.ds(w * STEP + step * tile, tile)
                        value = parts[slot, mine, h * states + s, span, :].astype(jnp.float32)
                        value = value + arrived[source, h * states + s, span, :].astype(jnp.float32)
                        planes.append(value)
                for v in range(width):
                    for t in range(states):
                        total = None
                        for w in range(width):
                            for s in range(states):
                                entry = pair_ref[((w * width + v) * states + s) * states + t]
                                term = planes[w * states + s] * entry
                                total = term if total is None else total + term
                        column = pl.multiple_of((v * blocks + h) * wide, wide)
                        mixed[target, pl.ds(t * STEP + step * tile, tile), pl.ds(column, wide)] = total.astype(
                            jnp.bfloat16
                        )
            return carry

        lax.fori_loop(0, blocks, one, 0)

    def up_copy(u, d):
        slot = lax.rem(u, DEPTH)
        return remote(sums.at[slot, d], from_low.at[slot, d], sum_send.at[slot, d], low_recv.at[slot, d], higher)

    def down_copy(u, d):
        slot = lax.rem(u, DEPTH)
        return remote(sums.at[slot, d], from_high.at[slot, d], sum_send.at[slot, d], high_recv.at[slot, d], lower)

    def drained(u):
        for d in range(line):

            @pl.when(d > place)
            def _():
                up_copy(u, d).wait_send()

            @pl.when(d < place)
            def _():
                down_copy(u, d).wait_send()

    def added(slot, d, source):
        total = sums[slot, d].astype(jnp.float32) + source[slot, d].astype(jnp.float32)
        sums[slot, d] = total.astype(jnp.bfloat16)

    def where_to(u):
        near = jnp.where(u < 2 * early, 1, 0)
        first = jnp.where(u < 3 * early, 1, 0)
        second = jnp.where(u < 6 * early, 1, 0)
        third = jnp.where(u < 8 * early, 1, 0)
        a, b, e, g = u, u - 2 * early, u - 3 * early, u - 6 * early
        f = u - 8 * early
        chunk = jnp.where(
            near == 1,
            a // 2,
            jnp.where(
                first == 1,
                b,
                jnp.where(second == 1, early + e // 3, jnp.where(third == 1, g, 2 * early + f // 4)),
            ),
        )
        kind = jnp.where(
            near == 1,
            lax.rem(a, 2),
            jnp.where(
                first == 1, 2, jnp.where(second == 1, lax.rem(e + 3 * units, 3), jnp.where(third == 1, 3, lax.rem(f + 8 * units, 4)))
            ),
        )
        return chunk, kind

    def done_copies(u):
        slot = lax.rem(u, 2)
        chunk, kind = where_to(u)
        far = kind // 2
        near_block = here + kind * (beside - here)
        copies = []
        for j in range(2):
            far_block = corner if j else across
            block = (1 - far) * near_block + far * far_block
            column = (1 - far) * j + far * (kind - 2)
            copies.append(
                pltpu.make_async_copy(
                    done.at[slot, j],
                    out_ref.at[
                        block,
                        :,
                        pl.ds(pl.multiple_of(chunk * STEP, STEP), STEP),
                        pl.ds(pl.multiple_of(column * half, half), half),
                    ],
                    done_sem.at[slot, j],
                )
            )
        return copies

    def handle(i):
        up = i - HOP * place
        slot_up = lax.rem(up + DEPTH * HOP * line, DEPTH)

        @pl.when(jnp.logical_and(place < line - 1, jnp.logical_and(up >= 0, up < units)))
        def _():
            @pl.when(up >= DEPTH)
            def _():
                pl.semaphore_wait(high_free, 1)

            for d in range(line - 1, 0, -1):

                @pl.when(d > place)
                def _():
                    @pl.when(place > 0)
                    def _():
                        up_copy(up, d).wait_recv()
                        added(slot_up, d, from_low)

                    up_copy(up, d).start()

        down = i - HOP * (line - 1 - place)
        slot_down = lax.rem(down + DEPTH * HOP * line, DEPTH)

        @pl.when(jnp.logical_and(place > 0, jnp.logical_and(down >= 0, down < units)))
        def _():
            @pl.when(down >= DEPTH)
            def _():
                pl.semaphore_wait(low_free, 1)

            for d in range(line - 1):

                @pl.when(d < place)
                def _():
                    @pl.when(place < line - 1)
                    def _():
                        down_copy(down, d).wait_recv()
                        added(slot_down, d, from_high)

                    down_copy(down, d).start()

        last = i - HOP * (line - 1)

        @pl.when(last >= 0)
        def _():
            slot = lax.rem(last, DEPTH)
            spot = lax.rem(last, 2)

            @pl.when(last >= 2)
            def _():
                for copy in done_copies(last - 2):
                    copy.wait()

            shape = done.shape[1:]
            value = sums[slot, place].astype(jnp.float32)
            done[spot] = value.reshape(shape)

            @pl.when(place > 0)
            def _():
                up_copy(last, place).wait_recv()
                more = from_low[slot, place].astype(jnp.float32)
                done[spot] = done[spot] + more.reshape(shape)

                @pl.when(last < units - DEPTH)
                def _():
                    pl.semaphore_signal(high_free, inc=1, device_id=lower, device_id_type=MESH)

            @pl.when(place < line - 1)
            def _():
                down_copy(last, place).wait_recv()
                more = from_high[slot, place].astype(jnp.float32)
                done[spot] = done[spot] + more.reshape(shape)

                @pl.when(last < units - DEPTH)
                def _():
                    pl.semaphore_signal(low_free, inc=1, device_id=higher, device_id_type=MESH)

            for copy in done_copies(last):
                copy.start()

    def unit(u, c, kind):
        slot = lax.rem(u, DEPTH)

        @pl.when(u >= DEPTH)
        def _():
            drained(u - DEPTH)

        source = lax.rem(c, DEPTH)

        def one(j, carry):
            value = jnp.dot(mixed[source], images[2 * kind + j], preferred_element_type=jnp.float32)
            value = value.astype(jnp.bfloat16)
            for d in range(line):
                sums[slot, d, j] = value[:, d * half : (d + 1) * half]
            return carry

        lax.fori_loop(0, 2, one, 0)
        handle(u)

    def walk(start, base, kinds, fresh):
        def one(n, carry):
            c = start + n
            if fresh:
                front(c)

            def inner(k, carry):
                unit(base + n * len(kinds) + k, c, kinds[0] + k)
                return carry

            lax.fori_loop(0, len(kinds), inner, 0)
            return carry

        return one

    left(0)
    for copy in beside_copies:
        copy.wait()
    lax.fori_loop(0, early, walk(0, 0, (0, 1), True), 0)
    across_copies[0].wait()
    corner_copies[0].start()
    corner_copies[0].wait()
    lax.fori_loop(0, early, walk(0, 2 * early, (2,), False), 0)
    lax.fori_loop(0, early, walk(early, 3 * early, (0, 1, 2), True), 0)
    across_copies[1].wait()
    corner_copies[1].start()
    corner_copies[1].wait()
    lax.fori_loop(0, 2 * early, walk(0, 6 * early, (3,), False), 0)
    lax.fori_loop(0, 2 * early, walk(2 * early, 8 * early, (0, 1, 2, 3), True), 0)

    def finish(i, carry):
        handle(i)
        return carry

    lax.fori_loop(units, units + HOP * (line - 1), finish, 0)
    for u in range(units - DEPTH, units):
        drained(u)
    for u in range(units - 2, units):
        for copy in done_copies(u):
            copy.wait()
    for c in range(chunks - 2, chunks):
        part_copy(c).wait_send()


def line_call(pair, own, near, far, env, right, line):
    pairs, depth, wide = own.shape
    chunks, rows, inner = env.shape
    width = rows // (2 * STEP)
    blocks = inner // depth
    states = pairs // blocks
    lanes = right.shape[1] // line
    half = lanes // 2
    tall = states * STEP
    low = jnp.bfloat16
    hbm = pl.BlockSpec(memory_space=pltpu.MemorySpace.HBM)
    dma = pltpu.SemaphoreType.DMA
    plain = pltpu.SemaphoreType.REGULAR
    return pl.pallas_call(
        functools.partial(line_kernel, (width, blocks, states, depth, line)),
        out_shape=jax.ShapeDtypeStruct((blocks, states, chunks * STEP, lanes), jnp.float32),
        in_specs=[pl.BlockSpec(memory_space=pltpu.SMEM)] + [hbm] * 5,
        out_specs=hbm,
        scratch_shapes=[
            pltpu.VMEM((pairs, inner, wide), low),
            pltpu.VMEM((8, right.shape[0], line * half), low),
            pltpu.VMEM((DEPTH, tall, right.shape[0]), low),
            pltpu.VMEM((2, rows, inner), low),
            pltpu.VMEM((2, 2, pairs, rows // 2, wide), low),
            pltpu.VMEM((4, pairs, rows // 2, wide), low),
            pltpu.VMEM((DEPTH, line, 2, tall, half), low),
            pltpu.VMEM((DEPTH, line, 2, tall, half), low),
            pltpu.VMEM((DEPTH, line, 2, tall, half), low),
            pltpu.VMEM((2, 2, states, STEP, half), jnp.float32),
            dma((3,)),
            dma((1,)),
            dma((1,)),
            dma((2, line)),
            dma((6,)),
            dma((6,)),
            dma((2,)),
            dma((2,)),
            dma((4,)),
            dma((DEPTH, line)),
            dma((DEPTH, line)),
            dma((DEPTH, line)),
            plain,
            plain,
            dma((2, 2)),
        ],
        compiler_params=pltpu.CompilerParams(
            collective_id=0, has_side_effects=True, vmem_limit_bytes=67043328
        ),
        cost_estimate=pl.CostEstimate(
            flops=2 * chunks * (rows * inner * pairs * wide + tall * right.shape[0] * 4 * line * lanes),
            bytes_accessed=2 * (env.size + 3 * own.size + right.size) + 4 * chunks * tall * blocks * lanes,
            transcendentals=0,
        ),
    )(pair.reshape(-1), own, near, far, env, right)


def lined_body(state, left_env, right_env, site_one, site_two):
    pair = pair_tensor(site_one, site_two)
    lefts, rights, owners = (lax.axis_size(name) for name in ("lb", "rb", "wa"))
    _, blocks, states, depth, lanes = state.shape
    entries = float(state.size * lefts * rights * owners)
    width, _, _, _, rows = left_env.shape
    own = state.reshape(blocks * states, depth, lanes)
    far = lax.ppermute(own, "wa", [(a, (a + 2) % 4) for a in range(owners)])
    near = lax.ppermute(own, "wa", [(a, a ^ 1) for a in range(owners)])
    chunks = rows // (lefts * STEP)
    env = left_env.reshape(width, blocks, depth, lefts, chunks, STEP)
    env = jnp.transpose(env, (4, 3, 0, 5, 1, 2)).reshape(chunks, lefts * width * STEP, blocks * depth)
    right = right_env.reshape(-1, right_env.shape[-1])
    applied = line_call(pair, own, near, far, env, right, rights)
    state_values = state[0].astype(jnp.float32)
    terms = jnp.stack(
        [
            jnp.sum(state_values * state_values),
            jnp.sum(state_values * applied),
            jnp.sum(applied * applied),
        ]
    )
    for name in ("wa", "lb", "rb"):
        size, bit = lax.axis_size(name), 1
        while bit < size:
            terms = terms + lax.ppermute(terms, name, [(a, a ^ bit) for a in range(size)])
            bit *= 2
    squares, crossed, image_squares = terms
    norm_sq = squares / entries + EPSILON
    projection = crossed / entries
    alpha_coef = projection / norm_sq
    beta_coef = jnp.sqrt((image_squares / entries - alpha_coef * projection) / norm_sq + EPSILON)
    scale = 1.0 / (jnp.sqrt(norm_sq) * beta_coef)
    result = (applied - alpha_coef * state_values) * scale
    return (result[None], jnp.stack([alpha_coef, beta_coef]))


def fits(mesh):
    return (mesh.shape["lb"], mesh.shape["rb"], mesh.shape["wa"]) == (2, 4, 4)


def solution(mesh):
    placed = (
        P("wa", None, None, "lb", "rb"),
        P(None, None, "lb", "wa", None),
        P(None, None, "rb", "wa", None),
        P(),
        P(),
    )
    if fits(mesh):
        return jax.shard_map(
            lined_body,
            mesh=mesh,
            in_specs=placed,
            out_specs=(P("wa", None, None, "lb", "rb"), P()),
            check_vma=False,
        )
    return jax.shard_map(
        body,
        mesh=mesh,
        in_specs=placed,
        out_specs=(P("wa", None, None, "lb", "rb"), P()),
        check_vma=False,
    )
```

```python
import functools
import jax
import jax.numpy as jnp
from jax import lax
from jax.experimental import pallas as pl
from jax.experimental.pallas import tpu as pltpu
from jax.sharding import PartitionSpec as P

EPSILON = 1e-06
CHUNKS = 4
GATHERS = 2


def pair_tensor(site_one, site_two):
    joined = jnp.einsum("wuac,uvbd->wvabcd", site_one, site_two, precision=lax.Precision.HIGHEST)
    mpo_width = site_one.shape[0]
    states = site_one.shape[2] * site_two.shape[2]
    return joined.reshape(mpo_width, mpo_width, states, states)


def mix_kernel(terms, pair_ref, *refs):
    out_ref = refs[terms]
    width, _, states, rows, _ = refs[0].shape
    step = 16

    @pl.loop(0, rows // step)
    def _(block):
        span = pl.ds(pl.multiple_of(block * step, step), step)
        planes = []
        for w in range(width):
            for s in range(states):
                value = refs[0][w, 0, s, span, :].astype(jnp.float32)
                for other in refs[1:terms]:
                    value = value + other[w, 0, s, span, :].astype(jnp.float32)
                planes.append(value)
        for v in range(width):
            for t in range(states):
                total = None
                for w in range(width):
                    for s in range(states):
                        entry = pair_ref[((w * width + v) * states + s) * states + t]
                        term = planes[w * states + s] * entry
                        total = term if total is None else total + term
                out_ref[v, 0, t, span, :] = total.astype(out_ref.dtype)


def mix(pair, parts):
    width, blocks, states, rows, lanes = parts[0].shape
    spec = pl.BlockSpec((width, 1, states, rows, lanes), lambda h: (0, h, 0, 0, 0))
    count = width * states
    size = parts[0].size
    return pl.pallas_call(
        functools.partial(mix_kernel, len(parts)),
        grid=(blocks,),
        out_shape=jax.ShapeDtypeStruct(parts[0].shape, jnp.bfloat16),
        in_specs=[pl.BlockSpec(memory_space=pltpu.SMEM)] + [spec] * len(parts),
        out_specs=spec,
        cost_estimate=pl.CostEstimate(
            flops=2 * size * count * 16, bytes_accessed=2 * size * (len(parts) + 1), transcendentals=0
        ),
    )(pair.reshape(-1), *parts)


def body(state, left_env, right_env, site_one, site_two):
    pair = pair_tensor(site_one, site_two)
    lefts, rights, owners = (lax.axis_size(name) for name in ("lb", "rb", "wa"))
    mine = lax.axis_index("lb")
    here = lax.axis_index("wa")
    _, blocks, _, _, _ = state.shape
    entries = float(state.size * lefts * rights * owners)

    group = blocks // GATHERS
    gathered = []
    for h in range(0, blocks, group):
        gathered.append(lax.all_gather(state[:, h : h + group], "wa", axis=0, tiled=True))
    turned = jnp.transpose(left_env[:, :, :, 0, :], (0, 1, 3, 2))
    owned = turned.shape[2] // lefts
    chunk = owned // CHUNKS

    def left_part(owner, position):
        rows = lax.dynamic_slice_in_dim(turned, owner * owned + position * chunk, chunk, 2)
        return [
            jnp.einsum(
                "wgpm,ghsmn->whspn", rows, part, preferred_element_type=jnp.float32
            ).astype(jnp.bfloat16)
            for part in gathered
        ]

    envs = {0: right_env[:, :, :, 0, :]}
    bit = owners // 2
    while bit:
        swap = [(a, a ^ bit) for a in range(owners)]
        for r in list(envs):
            envs[r ^ bit] = lax.ppermute(envs[r], "wa", swap)
        bit //= 2
    order = sorted(envs)
    near, far = order[: owners // 2], order[owners // 2 :]
    width, wide = envs[0].shape[0], envs[0].shape[3]

    def joined(pack):
        env = jnp.concatenate([envs[r] for r in pack], axis=3)
        return env.reshape(width, blocks, -1, len(pack), wide)

    packs = [(pack, joined(pack)) for pack in (near, far, order)]

    images = {r: [] for r in order}
    for position in range(CHUNKS):
        arrived = []
        for shift in range(1, lefts):
            sent = left_part(lax.rem(mine + shift, lefts), position)
            ring = [(a, (a + shift) % lefts) for a in range(lefts)]
            arrived.append([lax.ppermute(piece, "lb", ring) for piece in sent])
        parts = [jnp.concatenate(p, axis=1) for p in [left_part(mine, position)] + arrived]
        mixed = mix(pair, parts)
        for pack, env in packs[:2] if position == 0 else packs[2:]:
            part = jnp.einsum("vhtpn,vhndq->dtpq", mixed, env, preferred_element_type=jnp.float32).astype(jnp.bfloat16)
            part = lax.psum_scatter(part, "rb", scatter_dimension=3, tiled=True)
            for r, piece in zip(pack, part):
                images[r].append(piece)
    applied = [jnp.concatenate(images[r], axis=1).astype(jnp.float32) for r in order]
    vectors = [
        lax.dynamic_index_in_dim(state[0], here ^ r, 0, keepdims=False).astype(jnp.float32)
        for r in order
    ]
    state_values = state.astype(jnp.float32)
    terms = jnp.stack(
        [
            jnp.sum(state_values * state_values),
            sum(jnp.sum(s * a) for s, a in zip(vectors, applied)),
            sum(jnp.sum(a * a) for a in applied),
        ]
    )
    for name in ("wa", "lb", "rb"):
        size, bit = lax.axis_size(name), 1
        while bit < size:
            terms = terms + lax.ppermute(terms, name, [(a, a ^ bit) for a in range(size)])
            bit *= 2
    squares, crossed, image_squares = terms
    norm_sq = squares / entries + EPSILON
    projection = crossed / entries
    alpha_coef = projection / norm_sq
    beta_coef = jnp.sqrt((image_squares / entries - alpha_coef * projection) / norm_sq + EPSILON)
    scale = 1.0 / (jnp.sqrt(norm_sq) * beta_coef)
    result = jnp.zeros(state.shape, jnp.float32)
    for r, s, a in zip(order, vectors, applied):
        value = (a - alpha_coef * s) * scale
        result = lax.dynamic_update_slice(result, value[None, None], (0, here ^ r, 0, 0, 0))
    return (result, jnp.stack([alpha_coef, beta_coef]))


MESH = pl.DeviceIdType.MESH
STEP = 32
DEPTH = 8
HOP = 2
AHEAD = 3
LANES = 128


def line_kernel(
    sizes,
    pair_ref,
    own_ref,
    left_ref,
    right_ref,
    out_ref,
    env_ref,
    total_ref,
    psi,
    images,
    mixed,
    raw,
    rows_buf,
    parts,
    arrived,
    sums,
    from_low,
    from_high,
    done,
    terms,
    heard,
    load_sem,
    psi_send,
    psi_recv,
    relay_send,
    relay_recv,
    right_load,
    right_send,
    right_recv,
    raw_sem,
    turn_sem,
    rows_sem,
    part_send,
    part_recv,
    part_free,
    sum_send,
    low_recv,
    high_recv,
    low_free,
    high_free,
    done_sem,
    term_send,
    term_recv,
):
    width, blocks, states, depth, line, entries = sizes
    chunks = env_ref.shape[0]
    units = 4 * chunks
    early, middle = early_chunks(chunks)
    kept = early + middle
    inner = blocks * depth
    mine = lax.axis_index("lb")
    place = lax.axis_index("rb")
    here = lax.axis_index("wa")
    beside = here + 1 - 2 * lax.rem(here, 2)
    across = lax.rem(here + 2, 4)
    corner = 3 - here
    partner = (mine, place, beside)
    opposite = (mine, place, across)
    other = (1 - mine, place, here)
    higher = (mine, lax.rem(place + 1, line), here)
    lower = (mine, lax.rem(place + line - 1, line), here)
    paired = (mine, place + 1 - 2 * lax.rem(place, 2), here)
    distant = (mine, lax.rem(place + 2, line), here)

    def remote(source, target, send, recv, device):
        return pltpu.make_async_remote_copy(
            src_ref=source, dst_ref=target, send_sem=send, recv_sem=recv, device_id=device, device_id_type=MESH
        )

    my_span = pl.ds(pl.multiple_of(here * depth, depth), depth)
    across_span = pl.ds(pl.multiple_of(across * depth, depth), depth)
    own_copy = pltpu.make_async_copy(own_ref, psi.at[:, my_span, :], load_sem.at[0])
    own_copy.start()

    def raw_copy(n):
        slot = lax.rem(n, 2)
        q = n // (2 * width)
        side = lax.rem(n // width, 2)
        w = lax.rem(n, width)
        first = side * (chunks * STEP) + q * LANES
        return pltpu.make_async_copy(
            left_ref.at[pl.ds(pl.multiple_of(w * inner, inner), inner), pl.ds(pl.multiple_of(first, LANES), LANES)],
            raw.at[slot],
            raw_sem.at[slot],
        )

    raw_copy(0).start()

    barrier = pltpu.get_barrier_semaphore()
    devices = (partner, opposite, other, higher, lower, distant)
    for device in devices:
        pl.semaphore_signal(barrier, inc=1, device_id=device, device_id_type=MESH)
    pl.semaphore_wait(barrier, len(devices))

    def group(h):
        return pl.ds(h * states, states)

    psi_copies = [
        remote(own_ref.at[group(h)], psi.at[group(h), my_span, :], psi_send.at[h], psi_recv.at[h], opposite)
        for h in range(blocks)
    ]
    for copy in psi_copies:
        copy.start()
    share = remote(own_ref, psi.at[:, my_span, :], psi_send.at[blocks], psi_recv.at[blocks], partner)
    share.start()

    lanes = right_ref.shape[1] // line
    half = lanes // 2
    local = []
    for part in range(2):
        for d in range(line):
            local.append(
                pltpu.make_async_copy(
                    right_ref.at[:, pl.ds(d * lanes + part * half, half)],
                    images.at[part, :, pl.ds(d * half, half)],
                    right_load.at[part, d],
                )
            )
    for copy in local:
        copy.start()

    turns = 2 * width * chunks * STEP // LANES
    cuts = LANES // STEP

    def turned_copies(n):
        slot = lax.rem(n, 2)
        q = n // (2 * width)
        side = lax.rem(n // width, 2)
        w = lax.rem(n, width)
        first = (side * width + w) * STEP
        return [
            pltpu.make_async_copy(
                mixed.at[slot, pl.ds(k * STEP, STEP), pl.ds(0, inner)],
                env_ref.at[q * cuts + k, pl.ds(pl.multiple_of(first, STEP), STEP), :],
                turn_sem.at[slot, k],
            )
            for k in range(cuts)
        ]

    def turn(n, carry):
        slot = lax.rem(n, 2)

        @pl.when(n + 1 < turns)
        def _():
            raw_copy(n + 1).start()

        raw_copy(n).wait()

        @pl.when(n >= 2)
        def _():
            for copy in turned_copies(n - 2):
                copy.wait()

        for g in range(blocks):
            span = pl.ds(g * depth, depth)
            mixed[slot, pl.ds(0, LANES), span] = raw[slot, span, :].T
        for copy in turned_copies(n):
            copy.start()
        return carry

    lax.fori_loop(0, turns, turn, 0)
    for n in range(turns - 2, turns):
        for copy in turned_copies(n):
            copy.wait()

    def rows_copy(n, c):
        slot = lax.rem(n, 2)
        return pltpu.make_async_copy(env_ref.at[c], rows_buf.at[slot], rows_sem.at[slot])

    rows_copy(0, 0).start()
    own_copy.wait()
    terms[...] = jnp.zeros_like(terms)

    def folded(value):
        return jnp.sum(value.reshape(-1, 8, LANES), axis=0)

    def square(p, carry):
        value = psi[p, my_span, :].astype(jnp.float32)
        value = value * value
        for n in range(value.shape[1] // LANES):
            terms[0] += folded(value[:, n * LANES : (n + 1) * LANES])
        return carry

    lax.fori_loop(0, blocks * states, square, 0)
    for copy in local:
        copy.wait()

    def image_copy(n, source, target, device):
        return remote(images.at[source], images.at[target], right_send.at[n], right_recv.at[n], device)

    beside_copies = [image_copy(0, 0, 2, partner), image_copy(1, 1, 3, partner)]
    across_copies = [image_copy(2, 0, 4, opposite), image_copy(3, 1, 6, opposite)]
    corner_copies = [image_copy(4, 4, 5, partner), image_copy(5, 6, 7, partner)]

    def part_copy(c, h):
        slot = lax.rem(c, AHEAD)
        target = lax.rem(c, AHEAD + 1)
        return remote(
            parts.at[slot, 1 - mine, group(h)],
            arrived.at[target, group(h)],
            part_send.at[slot, h],
            part_recv.at[target, h],
            other,
        )

    def left_block(c, n, h):
        slot = lax.rem(c, AHEAD)
        source = lax.rem(n, 2)

        def one(s, carry):
            p = h * states + s
            value = jnp.dot(rows_buf[source], psi[p], preferred_element_type=jnp.float32)
            value = value.astype(jnp.bfloat16)
            rows = value.shape[0] // 2
            parts[slot, 0, p] = value[:rows]
            parts[slot, 1, p] = value[rows:]
            return carry

        lax.fori_loop(0, states, one, 0)
        part_copy(c, h).start()

    share.wait()
    for h in range(blocks):
        psi_copies[h].wait()
        if h == blocks - 1:
            for copy in across_copies:
                copy.start()
        relay = remote(
            psi.at[group(h), across_span, :], psi.at[group(h), across_span, :], relay_send.at[h], relay_recv.at[h], partner
        )
        relay.start()
        if h == 0:
            for copy in beside_copies:
                copy.start()
        relay.wait()

        def one(c, carry):
            n = h * AHEAD + c
            rows_copy(n, c).wait()
            rows_copy(n + 1, jnp.where(n == blocks * AHEAD - 1, AHEAD, lax.rem(c + 1, AHEAD))).start()
            left_block(c, n, h)
            return carry

        lax.fori_loop(0, AHEAD, one, 0)

    def left(c):
        n = c + (blocks - 1) * AHEAD
        for h in range(blocks):
            part_copy(c - AHEAD, h).wait_send()

        @pl.when(c > AHEAD)
        def _():
            pl.semaphore_wait(part_free, 1)

        rows_copy(n, c).wait()

        @pl.when(c + 1 < chunks)
        def _():
            rows_copy(n + 1, c + 1).start()

        for h in range(blocks):
            left_block(c, n, h)

    def front(c):
        slot = lax.rem(c, AHEAD)
        source = lax.rem(c, AHEAD + 1)
        target = lax.rem(c, kept)
        tile = 16
        wide = psi.shape[2]

        def one(h, carry):
            part_copy(c, h).wait_recv()
            for step in range(STEP // tile):
                planes = []
                for w in range(width):
                    for s in range(states):
                        span = pl.ds(w * STEP + step * tile, tile)
                        value = parts[slot, mine, h * states + s, span, :].astype(jnp.float32)
                        value = value + arrived[source, h * states + s, span, :].astype(jnp.float32)
                        planes.append(value)
                for v in range(width):
                    for t in range(states):
                        total = None
                        for w in range(width):
                            for s in range(states):
                                entry = pair_ref[((w * width + v) * states + s) * states + t]
                                term = planes[w * states + s] * entry
                                total = term if total is None else total + term
                        column = pl.multiple_of((v * blocks + h) * wide, wide)
                        mixed[target, pl.ds(t * STEP + step * tile, tile), pl.ds(column, wide)] = total.astype(
                            jnp.bfloat16
                        )
            return carry

        lax.fori_loop(0, blocks, one, 0)

        @pl.when(c + AHEAD + 1 < chunks)
        def _():
            pl.semaphore_signal(part_free, inc=1, device_id=other, device_id_type=MESH)

    def up_copy(u, d):
        slot = lax.rem(u, DEPTH)
        return remote(sums.at[slot, d], from_low.at[slot, d - 1], sum_send.at[slot, d], low_recv.at[slot, d - 1], higher)

    def down_copy(u, d):
        slot = lax.rem(u, DEPTH)
        return remote(sums.at[slot, d], from_high.at[slot, d], sum_send.at[slot, d], high_recv.at[slot, d], lower)

    def drained(u):
        for d in range(line):

            @pl.when(d > place)
            def _():
                up_copy(u, d).wait_send()

            @pl.when(d < place)
            def _():
                down_copy(u, d).wait_send()

    def added(slot, d, source, n):
        total = sums[slot, d].astype(jnp.float32) + source[slot, n].astype(jnp.float32)
        sums[slot, d] = total.astype(jnp.bfloat16)

    def where_to(u):
        second, third, fourth = 3 * early, 3 * early + 3 * middle, 4 * (early + middle)
        e, f = lax.rem(u + 3 * units - second, 3), lax.rem(u + 4 * units - fourth, 4)
        chunk = jnp.where(u < fourth, u - third, kept + (u - fourth) // 4)
        chunk = jnp.where(u < third, early + (u - second) // 3, chunk)
        chunk = jnp.where(u < second, u - 2 * early, chunk)
        chunk = jnp.where(u < 2 * early, u // 2, chunk)
        kind = jnp.where(u < fourth, 3, f)
        kind = jnp.where(u < third, e, kind)
        kind = jnp.where(u < second, 2, kind)
        kind = jnp.where(u < 2 * early, lax.rem(u, 2), kind)
        return chunk, kind

    def places(u):
        chunk, kind = where_to(u)
        far = kind // 2
        near_block = here + kind * (beside - here)
        spots = []
        for j in range(2):
            far_block = corner if j else across
            block = (1 - far) * near_block + far * far_block
            column = (1 - far) * j + far * (kind - 2)
            spots.append((block, column))
        return chunk, spots

    def done_copies(u):
        slot = lax.rem(u, 2)
        chunk, spots = places(u)
        copies = []
        for j, (block, column) in enumerate(spots):
            copies.append(
                pltpu.make_async_copy(
                    done.at[slot, j],
                    out_ref.at[
                        block,
                        :,
                        pl.ds(pl.multiple_of(chunk * STEP, STEP), STEP),
                        pl.ds(pl.multiple_of(column * half, half), half),
                    ],
                    done_sem.at[slot, j],
                )
            )
        return copies

    def gather_terms(u):
        slot = lax.rem(u, 2)
        chunk, spots = places(u)
        first = pl.multiple_of(here * depth + chunk * STEP, STEP)
        for j, (block, column) in enumerate(spots):
            for t in range(states):
                value = done[slot, j, t]
                start = psi[block * states + t, pl.ds(first, STEP), pl.ds(pl.multiple_of(column * half, half), half)]
                start = start.astype(jnp.float32)
                terms[1] += folded(start * value)
                terms[2] += folded(value * value)

    def handle(i):
        up = i - HOP * place
        slot_up = lax.rem(up + DEPTH * HOP * line, DEPTH)

        @pl.when(jnp.logical_and(place < line - 1, jnp.logical_and(up >= 0, up < units)))
        def _():
            @pl.when(up >= DEPTH)
            def _():
                pl.semaphore_wait(high_free, 1)

            for d in range(line - 1, 0, -1):

                @pl.when(d > place)
                def _():
                    @pl.when(place > 0)
                    def _():
                        up_copy(up, d).wait_recv()
                        added(slot_up, d, from_low, d - 1)

                    up_copy(up, d).start()

        down = i - HOP * (line - 1 - place)
        slot_down = lax.rem(down + DEPTH * HOP * line, DEPTH)

        @pl.when(jnp.logical_and(place > 0, jnp.logical_and(down >= 0, down < units)))
        def _():
            @pl.when(down >= DEPTH)
            def _():
                pl.semaphore_wait(low_free, 1)

            for d in range(line - 1):

                @pl.when(d < place)
                def _():
                    @pl.when(place < line - 1)
                    def _():
                        down_copy(down, d).wait_recv()
                        added(slot_down, d, from_high, d)

                    down_copy(down, d).start()

        last = i - HOP * (line - 1)

        @pl.when(last >= 0)
        def _():
            slot = lax.rem(last, DEPTH)
            spot = lax.rem(last, 2)

            @pl.when(last >= 2)
            def _():
                for copy in done_copies(last - 2):
                    copy.wait()

            shape = done.shape[1:]
            value = sums[slot, place].astype(jnp.float32)
            done[spot] = value.reshape(shape)

            @pl.when(place > 0)
            def _():
                up_copy(last, place).wait_recv()
                more = from_low[slot, place - 1].astype(jnp.float32)
                done[spot] = done[spot] + more.reshape(shape)

                @pl.when(last < units - DEPTH)
                def _():
                    pl.semaphore_signal(high_free, inc=1, device_id=lower, device_id_type=MESH)

            @pl.when(place < line - 1)
            def _():
                down_copy(last, place).wait_recv()
                more = from_high[slot, place].astype(jnp.float32)
                done[spot] = done[spot] + more.reshape(shape)

                @pl.when(last < units - DEPTH)
                def _():
                    pl.semaphore_signal(low_free, inc=1, device_id=higher, device_id_type=MESH)

            for copy in done_copies(last):
                copy.start()
            gather_terms(last)

    def unit(u, c, kind):
        slot = lax.rem(u, DEPTH)

        @pl.when(u >= DEPTH)
        def _():
            drained(u - DEPTH)

        source = lax.rem(c, kept)

        def one(j, carry):
            value = jnp.dot(mixed[source], images[2 * kind + j], preferred_element_type=jnp.float32)
            value = value.astype(jnp.bfloat16)
            for d in range(line):
                sums[slot, d, j] = value[:, d * half : (d + 1) * half]
            return carry

        lax.fori_loop(0, 2, one, 0)
        handle(u)

    def walk(start, base, kinds, fresh):
        def one(n, carry):
            c = start + n
            if fresh:
                front(c)

            def inner(k, carry):
                unit(base + n * len(kinds) + k, c, kinds[0] + k)
                return carry

            lax.fori_loop(0, len(kinds), inner, 0)
            if fresh:

                @pl.when(c + AHEAD < chunks)
                def _():
                    left(c + AHEAD)

            return carry

        return one

    for copy in beside_copies:
        copy.wait()
    lax.fori_loop(0, early, walk(0, 0, (0, 1), True), 0)
    across_copies[0].wait()
    corner_copies[0].start()
    corner_copies[0].wait()
    lax.fori_loop(0, early, walk(0, 2 * early, (2,), False), 0)
    lax.fori_loop(0, middle, walk(early, 3 * early, (0, 1, 2), True), 0)
    across_copies[1].wait()
    corner_copies[1].start()
    corner_copies[1].wait()
    lax.fori_loop(0, kept, walk(0, 3 * kept, (3,), False), 0)
    lax.fori_loop(0, chunks - kept, walk(kept, 4 * kept, (0, 1, 2, 3), True), 0)

    def finish(i, carry):
        handle(i)
        return carry

    lax.fori_loop(units, units + HOP * (line - 1), finish, 0)
    for n, device in enumerate((partner, opposite, other, paired, distant)):
        copy = remote(terms, heard.at[n], term_send.at[n], term_recv.at[n], device)
        copy.start()
        copy.wait()
        terms[...] = terms[...] + heard[n]

    def whole(n):
        value = jnp.sum(terms[n], axis=1, keepdims=True)
        return jnp.sum(value, axis=0, keepdims=True) / entries

    norm_sq = whole(0) + EPSILON
    projection = whole(1)
    alpha_coef = projection / norm_sq
    beta_coef = jnp.sqrt((whole(2) - alpha_coef * projection) / norm_sq + EPSILON)
    scale = 1.0 / (jnp.sqrt(norm_sq) * beta_coef)
    for n, value in enumerate((alpha_coef, beta_coef, scale)):
        total_ref[n] = jnp.broadcast_to(value, total_ref.shape[1:])
    for u in range(units - DEPTH, units):
        drained(u)
    for u in range(units - 2, units):
        for copy in done_copies(u):
            copy.wait()
    for c in range(chunks - AHEAD, chunks):
        for h in range(blocks):
            part_copy(c, h).wait_send()


def early_chunks(chunks):
    return 6 * chunks // 16, 3 * chunks // 16


def line_call(pair, own, left, right, line, lefts, blocks, entries):
    pairs, depth, wide = own.shape
    states = pairs // blocks
    inner = blocks * depth
    width = left.shape[0] // inner
    chunks = left.shape[1] // (lefts * STEP)
    rows = lefts * width * STEP
    lanes = right.shape[1] // line
    half = lanes // 2
    tall = states * STEP
    low = jnp.bfloat16
    hbm = pl.BlockSpec(memory_space=pltpu.MemorySpace.HBM)
    dma = pltpu.SemaphoreType.DMA
    plain = pltpu.SemaphoreType.REGULAR
    return pl.pallas_call(
        functools.partial(line_kernel, (width, blocks, states, depth, line, entries)),
        out_shape=(
            jax.ShapeDtypeStruct((blocks, states, chunks * STEP, lanes), jnp.float32),
            jax.ShapeDtypeStruct((chunks, rows, inner), low),
            jax.ShapeDtypeStruct((3, 8, LANES), jnp.float32),
        ),
        in_specs=[pl.BlockSpec(memory_space=pltpu.SMEM)] + [hbm] * 3,
        out_specs=(hbm, hbm, pl.BlockSpec(memory_space=pltpu.VMEM)),
        scratch_shapes=[
            pltpu.VMEM((pairs, inner, wide), low),
            pltpu.VMEM((8, right.shape[0], line * half), low),
            pltpu.VMEM((sum(early_chunks(chunks)), tall, right.shape[0]), low),
            pltpu.VMEM((2, inner, LANES), low),
            pltpu.VMEM((2, rows, inner), low),
            pltpu.VMEM((AHEAD, 2, pairs, rows // 2, wide), low),
            pltpu.VMEM((AHEAD + 1, pairs, rows // 2, wide), low),
            pltpu.VMEM((DEPTH, line, 2, tall, half), low),
            pltpu.VMEM((DEPTH, line - 1, 2, tall, half), low),
            pltpu.VMEM((DEPTH, line - 1, 2, tall, half), low),
            pltpu.VMEM((2, 2, states, STEP, half), jnp.float32),
            pltpu.VMEM((3, 8, LANES), jnp.float32),
            pltpu.VMEM((5, 3, 8, LANES), jnp.float32),
            dma((1,)),
            dma((blocks + 1,)),
            dma((blocks + 1,)),
            dma((blocks,)),
            dma((blocks,)),
            dma((2, line)),
            dma((6,)),
            dma((6,)),
            dma((2,)),
            dma((2, LANES // STEP)),
            dma((2,)),
            dma((AHEAD, blocks)),
            dma((AHEAD + 1, blocks)),
            plain,
            dma((DEPTH, line)),
            dma((DEPTH, line - 1)),
            dma((DEPTH, line - 1)),
            plain,
            plain,
            dma((2, 2)),
            dma((5,)),
            dma((5,)),
        ],
        compiler_params=pltpu.CompilerParams(
            collective_id=0, has_side_effects=True, vmem_limit_bytes=67043328
        ),
        cost_estimate=pl.CostEstimate(
            flops=2 * chunks * (rows * inner * pairs * wide + tall * right.shape[0] * 4 * line * lanes),
            bytes_accessed=4 * (left.size + own.size + right.size) + 4 * chunks * tall * blocks * lanes,
            transcendentals=0,
        ),
    )(pair.reshape(-1), own, left, right)


def lined_body(state, left_env, right_env, site_one, site_two):
    pair = pair_tensor(site_one, site_two)
    lefts, rights, owners = (lax.axis_size(name) for name in ("lb", "rb", "wa"))
    _, blocks, states, depth, lanes = state.shape
    entries = float(state.size * lefts * rights * owners)
    own = state.reshape(blocks * states, depth, lanes)
    left = left_env.reshape(-1, left_env.shape[-1])
    right = right_env.reshape(-1, right_env.shape[-1])
    applied, _, totals = line_call(pair, own, left, right, rights, lefts, blocks, entries)
    alpha_coef, beta_coef, scale = totals[0, 0, 0], totals[1, 0, 0], totals[2, 0, 0]
    result = (applied - alpha_coef * state[0].astype(jnp.float32)) * scale
    return (result[None], jnp.stack([alpha_coef, beta_coef]))


def fits(mesh):
    return (mesh.shape["lb"], mesh.shape["rb"], mesh.shape["wa"]) == (2, 4, 4)


def solution(mesh):
    placed = (
        P("wa", None, None, "lb", "rb"),
        P(None, None, "lb", "wa", None),
        P(None, None, "rb", "wa", None),
        P(),
        P(),
    )
    if fits(mesh):
        return jax.shard_map(
            lined_body,
            mesh=mesh,
            in_specs=placed,
            out_specs=(P("wa", None, None, "lb", "rb"), P()),
            check_vma=False,
        )
    return jax.shard_map(
        body,
        mesh=mesh,
        in_specs=placed,
        out_specs=(P("wa", None, None, "lb", "rb"), P()),
        check_vma=False,
    )
```

```python
import functools
import jax
import jax.numpy as jnp
from jax import lax
from jax.experimental import pallas as pl
from jax.experimental.pallas import tpu as pltpu
from jax.sharding import PartitionSpec as P

EPSILON = 1e-06
CHUNKS = 4
GATHERS = 2


def pair_tensor(site_one, site_two):
    joined = jnp.einsum("wuac,uvbd->wvabcd", site_one, site_two, precision=lax.Precision.HIGHEST)
    mpo_width = site_one.shape[0]
    states = site_one.shape[2] * site_two.shape[2]
    return joined.reshape(mpo_width, mpo_width, states, states)


def mix_kernel(terms, pair_ref, *refs):
    out_ref = refs[terms]
    width, _, states, rows, _ = refs[0].shape
    step = 16

    @pl.loop(0, rows // step)
    def _(block):
        span = pl.ds(pl.multiple_of(block * step, step), step)
        planes = []
        for w in range(width):
            for s in range(states):
                value = refs[0][w, 0, s, span, :].astype(jnp.float32)
                for other in refs[1:terms]:
                    value = value + other[w, 0, s, span, :].astype(jnp.float32)
                planes.append(value)
        for v in range(width):
            for t in range(states):
                total = None
                for w in range(width):
                    for s in range(states):
                        entry = pair_ref[((w * width + v) * states + s) * states + t]
                        term = planes[w * states + s] * entry
                        total = term if total is None else total + term
                out_ref[v, 0, t, span, :] = total.astype(out_ref.dtype)


def mix(pair, parts):
    width, blocks, states, rows, lanes = parts[0].shape
    spec = pl.BlockSpec((width, 1, states, rows, lanes), lambda h: (0, h, 0, 0, 0))
    count = width * states
    size = parts[0].size
    return pl.pallas_call(
        functools.partial(mix_kernel, len(parts)),
        grid=(blocks,),
        out_shape=jax.ShapeDtypeStruct(parts[0].shape, jnp.bfloat16),
        in_specs=[pl.BlockSpec(memory_space=pltpu.SMEM)] + [spec] * len(parts),
        out_specs=spec,
        cost_estimate=pl.CostEstimate(
            flops=2 * size * count * 16, bytes_accessed=2 * size * (len(parts) + 1), transcendentals=0
        ),
    )(pair.reshape(-1), *parts)


def body(state, left_env, right_env, site_one, site_two):
    pair = pair_tensor(site_one, site_two)
    lefts, rights, owners = (lax.axis_size(name) for name in ("lb", "rb", "wa"))
    mine = lax.axis_index("lb")
    here = lax.axis_index("wa")
    _, blocks, _, _, _ = state.shape
    entries = float(state.size * lefts * rights * owners)

    group = blocks // GATHERS
    gathered = []
    for h in range(0, blocks, group):
        gathered.append(lax.all_gather(state[:, h : h + group], "wa", axis=0, tiled=True))
    turned = jnp.transpose(left_env[:, :, :, 0, :], (0, 1, 3, 2))
    owned = turned.shape[2] // lefts
    chunk = owned // CHUNKS

    def left_part(owner, position):
        rows = lax.dynamic_slice_in_dim(turned, owner * owned + position * chunk, chunk, 2)
        return [
            jnp.einsum(
                "wgpm,ghsmn->whspn", rows, part, preferred_element_type=jnp.float32
            ).astype(jnp.bfloat16)
            for part in gathered
        ]

    envs = {0: right_env[:, :, :, 0, :]}
    bit = owners // 2
    while bit:
        swap = [(a, a ^ bit) for a in range(owners)]
        for r in list(envs):
            envs[r ^ bit] = lax.ppermute(envs[r], "wa", swap)
        bit //= 2
    order = sorted(envs)
    near, far = order[: owners // 2], order[owners // 2 :]
    width, wide = envs[0].shape[0], envs[0].shape[3]

    def joined(pack):
        env = jnp.concatenate([envs[r] for r in pack], axis=3)
        return env.reshape(width, blocks, -1, len(pack), wide)

    packs = [(pack, joined(pack)) for pack in (near, far, order)]

    images = {r: [] for r in order}
    for position in range(CHUNKS):
        arrived = []
        for shift in range(1, lefts):
            sent = left_part(lax.rem(mine + shift, lefts), position)
            ring = [(a, (a + shift) % lefts) for a in range(lefts)]
            arrived.append([lax.ppermute(piece, "lb", ring) for piece in sent])
        parts = [jnp.concatenate(p, axis=1) for p in [left_part(mine, position)] + arrived]
        mixed = mix(pair, parts)
        for pack, env in packs[:2] if position == 0 else packs[2:]:
            part = jnp.einsum("vhtpn,vhndq->dtpq", mixed, env, preferred_element_type=jnp.float32).astype(jnp.bfloat16)
            part = lax.psum_scatter(part, "rb", scatter_dimension=3, tiled=True)
            for r, piece in zip(pack, part):
                images[r].append(piece)
    applied = [jnp.concatenate(images[r], axis=1).astype(jnp.float32) for r in order]
    vectors = [
        lax.dynamic_index_in_dim(state[0], here ^ r, 0, keepdims=False).astype(jnp.float32)
        for r in order
    ]
    state_values = state.astype(jnp.float32)
    terms = jnp.stack(
        [
            jnp.sum(state_values * state_values),
            sum(jnp.sum(s * a) for s, a in zip(vectors, applied)),
            sum(jnp.sum(a * a) for a in applied),
        ]
    )
    for name in ("wa", "lb", "rb"):
        size, bit = lax.axis_size(name), 1
        while bit < size:
            terms = terms + lax.ppermute(terms, name, [(a, a ^ bit) for a in range(size)])
            bit *= 2
    squares, crossed, image_squares = terms
    norm_sq = squares / entries + EPSILON
    projection = crossed / entries
    alpha_coef = projection / norm_sq
    beta_coef = jnp.sqrt((image_squares / entries - alpha_coef * projection) / norm_sq + EPSILON)
    scale = 1.0 / (jnp.sqrt(norm_sq) * beta_coef)
    result = jnp.zeros(state.shape, jnp.float32)
    for r, s, a in zip(order, vectors, applied):
        value = (a - alpha_coef * s) * scale
        result = lax.dynamic_update_slice(result, value[None, None], (0, here ^ r, 0, 0, 0))
    return (result, jnp.stack([alpha_coef, beta_coef]))


MESH = pl.DeviceIdType.MESH
STEP = 32
DEPTH = 8
HOP = 2
AHEAD = 4
CUT = 2
LANES = 128


def line_kernel(
    sizes,
    pair_ref,
    own_ref,
    left_ref,
    right_ref,
    out_ref,
    env_ref,
    total_ref,
    psi,
    images,
    mixed,
    raw,
    rows_buf,
    parts,
    arrived,
    sums,
    from_low,
    from_high,
    done,
    ready,
    terms,
    heard,
    load_sem,
    psi_send,
    psi_recv,
    relay_send,
    relay_recv,
    right_load,
    right_send,
    right_recv,
    raw_sem,
    turn_sem,
    rows_sem,
    part_send,
    part_recv,
    part_free,
    sum_send,
    low_recv,
    high_recv,
    low_free,
    high_free,
    done_sem,
    term_send,
    term_recv,
):
    width, blocks, states, depth, line, entries = sizes
    chunks = env_ref.shape[0]
    units = 4 * chunks
    early, middle = early_chunks(chunks)
    kept = early + middle
    inner = blocks * depth
    piece = inner // CUT
    mine = lax.axis_index("lb")
    place = lax.axis_index("rb")
    here = lax.axis_index("wa")
    beside = here + 1 - 2 * lax.rem(here, 2)
    across = lax.rem(here + 2, 4)
    corner = 3 - here
    partner = (mine, place, beside)
    opposite = (mine, place, across)
    other = (1 - mine, place, here)
    higher = (mine, lax.rem(place + 1, line), here)
    lower = (mine, lax.rem(place + line - 1, line), here)
    turned_line = [(mine, lax.rem(place + k, line), here) for k in range(1, line)]
    turned_blocks = [(mine, place, lax.rem(here + k, 4)) for k in range(1, 4)]

    def remote(source, target, send, recv, device):
        return pltpu.make_async_remote_copy(
            src_ref=source, dst_ref=target, send_sem=send, recv_sem=recv, device_id=device, device_id_type=MESH
        )

    my_span = pl.ds(pl.multiple_of(here * depth, depth), depth)
    across_span = pl.ds(pl.multiple_of(across * depth, depth), depth)
    own_copy = pltpu.make_async_copy(own_ref, psi.at[:, my_span, :], load_sem.at[0])
    own_copy.start()

    def raw_copy(n):
        slot = lax.rem(n, 2)
        q = n // (2 * width * CUT)
        side = lax.rem(n // (width * CUT), 2)
        row = lax.rem(n, width * CUT) * piece
        first = side * (chunks * STEP) + q * LANES
        return pltpu.make_async_copy(
            left_ref.at[pl.ds(pl.multiple_of(row, piece), piece), pl.ds(pl.multiple_of(first, LANES), LANES)],
            raw.at[slot],
            raw_sem.at[slot],
        )

    raw_copy(0).start()

    barrier = pltpu.get_barrier_semaphore()
    devices = turned_line + turned_blocks + [other]
    for device in devices:
        pl.semaphore_signal(barrier, inc=1, device_id=device, device_id_type=MESH)
    pl.semaphore_wait(barrier, len(devices))

    def group(h):
        return pl.ds(h * states, states)

    psi_copies = [
        remote(own_ref.at[group(h)], psi.at[group(h), my_span, :], psi_send.at[h], psi_recv.at[h], opposite)
        for h in range(blocks)
    ]
    for copy in psi_copies:
        copy.start()
    share = remote(own_ref, psi.at[:, my_span, :], psi_send.at[blocks], psi_recv.at[blocks], partner)
    share.start()

    lanes = right_ref.shape[1] // line
    half = lanes // 2
    local = []
    for part in range(2):
        for d in range(line):
            local.append(
                pltpu.make_async_copy(
                    right_ref.at[:, pl.ds(d * lanes + part * half, half)],
                    images.at[part, :, pl.ds(d * half, half)],
                    right_load.at[part, d],
                )
            )
    for copy in local:
        copy.start()

    turns = 2 * width * CUT * chunks * STEP // LANES
    cuts = LANES // STEP

    def turned_copies(n):
        slot = lax.rem(n, 2)
        q = n // (2 * width * CUT)
        side = lax.rem(n // (width * CUT), 2)
        w = lax.rem(n // CUT, width)
        first = (side * width + w) * STEP
        column = pl.multiple_of(lax.rem(n, CUT) * piece, piece)
        return [
            pltpu.make_async_copy(
                mixed.at[slot, pl.ds(k * STEP, STEP), pl.ds(0, piece)],
                env_ref.at[q * cuts + k, pl.ds(pl.multiple_of(first, STEP), STEP), pl.ds(column, piece)],
                turn_sem.at[slot, k],
            )
            for k in range(cuts)
        ]

    def turn(n, carry):
        slot = lax.rem(n, 2)

        @pl.when(n + 1 < turns)
        def _():
            raw_copy(n + 1).start()

        raw_copy(n).wait()

        @pl.when(n >= 2)
        def _():
            for copy in turned_copies(n - 2):
                copy.wait()

        for g in range(blocks // CUT):
            span = pl.ds(g * depth, depth)
            mixed[slot, pl.ds(0, LANES), span] = raw[slot, span, :].T
        for copy in turned_copies(n):
            copy.start()
        return carry

    lax.fori_loop(0, turns, turn, 0)
    for n in range(turns - 2, turns):
        for copy in turned_copies(n):
            copy.wait()

    def rows_copy(n, c):
        slot = lax.rem(n, 2)
        return pltpu.make_async_copy(env_ref.at[c], rows_buf.at[slot], rows_sem.at[slot])

    rows_copy(0, 0).start()
    own_copy.wait()
    terms[...] = jnp.zeros_like(terms)

    def folded(value):
        return jnp.sum(value.reshape(-1, 8, LANES), axis=0)

    def square(p, carry):
        value = psi[p, my_span, :].astype(jnp.float32)
        value = value * value
        for n in range(value.shape[1] // LANES):
            terms[0] += folded(value[:, n * LANES : (n + 1) * LANES])
        return carry

    lax.fori_loop(0, blocks * states, square, 0)
    for copy in local:
        copy.wait()

    def image_copy(n, source, target, device):
        return remote(images.at[source], images.at[target], right_send.at[n], right_recv.at[n], device)

    beside_copies = [image_copy(0, 0, 2, partner), image_copy(1, 1, 3, partner)]
    across_copies = [image_copy(2, 0, 4, opposite), image_copy(3, 1, 6, opposite)]
    corner_copies = [image_copy(4, 4, 5, partner), image_copy(5, 6, 7, partner)]

    def part_copy(c, h):
        slot = lax.rem(c, AHEAD)
        target = lax.rem(c, AHEAD)
        return remote(
            parts.at[slot, 1 - mine, group(h)],
            arrived.at[target, group(h)],
            part_send.at[slot, h],
            part_recv.at[target, h],
            other,
        )

    def left_block(c, n, h):
        slot = lax.rem(c, AHEAD)
        source = lax.rem(n, 2)

        def one(s, carry):
            p = h * states + s
            value = jnp.dot(rows_buf[source], psi[p], preferred_element_type=jnp.float32)
            value = value.astype(jnp.bfloat16)
            rows = value.shape[0] // 2
            parts[slot, 0, p] = value[:rows]
            parts[slot, 1, p] = value[rows:]
            return carry

        lax.fori_loop(0, states, one, 0)
        part_copy(c, h).start()

    share.wait()
    for h in range(blocks):
        psi_copies[h].wait()
        if h == blocks - 1:
            for copy in across_copies:
                copy.start()
        relay = remote(
            psi.at[group(h), across_span, :], psi.at[group(h), across_span, :], relay_send.at[h], relay_recv.at[h], partner
        )
        relay.start()
        if h == 0:
            for copy in beside_copies:
                copy.start()
        relay.wait()

        def one(c, carry):
            n = h * AHEAD + c
            rows_copy(n, c).wait()
            rows_copy(n + 1, jnp.where(n == blocks * AHEAD - 1, AHEAD, lax.rem(c + 1, AHEAD))).start()
            left_block(c, n, h)
            return carry

        lax.fori_loop(0, AHEAD, one, 0)

    def left(c):
        n = c + (blocks - 1) * AHEAD
        for h in range(blocks):
            part_copy(c - AHEAD, h).wait_send()

        pl.semaphore_wait(part_free, 1)
        rows_copy(n, c).wait()

        @pl.when(c + 1 < chunks)
        def _():
            rows_copy(n + 1, c + 1).start()

        for h in range(blocks):
            left_block(c, n, h)

    def front(c):
        slot = lax.rem(c, AHEAD)
        source = lax.rem(c, AHEAD)
        target = lax.rem(c, kept)
        tile = 16
        wide = psi.shape[2]

        def one(h, carry):
            part_copy(c, h).wait_recv()
            for step in range(STEP // tile):
                planes = []
                for w in range(width):
                    for s in range(states):
                        span = pl.ds(w * STEP + step * tile, tile)
                        value = parts[slot, mine, h * states + s, span, :].astype(jnp.float32)
                        value = value + arrived[source, h * states + s, span, :].astype(jnp.float32)
                        planes.append(value)
                for v in range(width):
                    for t in range(states):
                        total = None
                        for w in range(width):
                            for s in range(states):
                                entry = pair_ref[((w * width + v) * states + s) * states + t]
                                term = planes[w * states + s] * entry
                                total = term if total is None else total + term
                        column = pl.multiple_of((v * blocks + h) * wide, wide)
                        mixed[target, pl.ds(t * STEP + step * tile, tile), pl.ds(column, wide)] = total.astype(
                            jnp.bfloat16
                        )
            return carry

        lax.fori_loop(0, blocks, one, 0)

        @pl.when(c + AHEAD < chunks)
        def _():
            pl.semaphore_signal(part_free, inc=1, device_id=other, device_id_type=MESH)

    def up_copy(u, d):
        slot = lax.rem(u, DEPTH)
        return remote(sums.at[slot, d], from_low.at[slot, d - 1], sum_send.at[slot, d], low_recv.at[slot, d - 1], higher)

    def down_copy(u, d):
        slot = lax.rem(u, DEPTH)
        return remote(sums.at[slot, d], from_high.at[slot, d], sum_send.at[slot, d], high_recv.at[slot, d], lower)

    def drained(u):
        for d in range(line):

            @pl.when(d > place)
            def _():
                up_copy(u, d).wait_send()

            @pl.when(d < place)
            def _():
                down_copy(u, d).wait_send()

    def added(slot, d, source, n):
        total = sums[slot, d].astype(jnp.float32) + source[slot, n].astype(jnp.float32)
        sums[slot, d] = total.astype(jnp.bfloat16)

    def where_to(u):
        second, third, fourth = 3 * early, 3 * early + 3 * middle, 4 * (early + middle)
        e, f = lax.rem(u + 3 * units - second, 3), lax.rem(u + 4 * units - fourth, 4)
        chunk = jnp.where(u < fourth, u - third, kept + (u - fourth) // 4)
        chunk = jnp.where(u < third, early + (u - second) // 3, chunk)
        chunk = jnp.where(u < second, u - 2 * early, chunk)
        chunk = jnp.where(u < 2 * early, u // 2, chunk)
        kind = jnp.where(u < fourth, 3, f)
        kind = jnp.where(u < third, e, kind)
        kind = jnp.where(u < second, 2, kind)
        kind = jnp.where(u < 2 * early, lax.rem(u, 2), kind)
        return chunk, kind

    def places(u):
        chunk, kind = where_to(u)
        far = kind // 2
        near_block = here + kind * (beside - here)
        spots = []
        for j in range(2):
            far_block = corner if j else across
            block = (1 - far) * near_block + far * far_block
            column = (1 - far) * j + far * (kind - 2)
            spots.append((block, column))
        return chunk, spots

    def done_copies(u):
        slot = lax.rem(u, 2)
        chunk, spots = places(u)
        copies = []
        for j, (block, column) in enumerate(spots):
            copies.append(
                pltpu.make_async_copy(
                    ready.at[slot, j],
                    out_ref.at[
                        block,
                        :,
                        pl.ds(pl.multiple_of(chunk * STEP, STEP), STEP),
                        pl.ds(pl.multiple_of(column * half, half), half),
                    ],
                    done_sem.at[slot, j],
                )
            )
        return copies

    def gather_terms(u):
        slot = lax.rem(u, 2)
        chunk, spots = places(u)
        first = pl.multiple_of(here * depth + chunk * STEP, STEP)
        for j, (block, column) in enumerate(spots):
            for t in range(states):
                value = done[j, t]
                ready[slot, j, t] = value.astype(ready.dtype)
                start = psi[block * states + t, pl.ds(first, STEP), pl.ds(pl.multiple_of(column * half, half), half)]
                start = start.astype(jnp.float32)
                terms[1] += folded(start * value)
                terms[2] += folded(value * value)

    def handle(i):
        up = i - HOP * place
        slot_up = lax.rem(up + DEPTH * HOP * line, DEPTH)

        @pl.when(jnp.logical_and(place < line - 1, jnp.logical_and(up >= 0, up < units)))
        def _():
            @pl.when(up >= DEPTH)
            def _():
                pl.semaphore_wait(high_free, 1)

            for d in range(line - 1, 0, -1):

                @pl.when(d > place)
                def _():
                    @pl.when(place > 0)
                    def _():
                        up_copy(up, d).wait_recv()
                        added(slot_up, d, from_low, d - 1)

                    up_copy(up, d).start()

        down = i - HOP * (line - 1 - place)
        slot_down = lax.rem(down + DEPTH * HOP * line, DEPTH)

        @pl.when(jnp.logical_and(place > 0, jnp.logical_and(down >= 0, down < units)))
        def _():
            @pl.when(down >= DEPTH)
            def _():
                pl.semaphore_wait(low_free, 1)

            for d in range(line - 1):

                @pl.when(d < place)
                def _():
                    @pl.when(place < line - 1)
                    def _():
                        down_copy(down, d).wait_recv()
                        added(slot_down, d, from_high, d)

                    down_copy(down, d).start()

        last = i - HOP * (line - 1)

        @pl.when(last >= 0)
        def _():
            slot = lax.rem(last, DEPTH)

            @pl.when(last >= 2)
            def _():
                for copy in done_copies(last - 2):
                    copy.wait()

            shape = done.shape
            value = sums[slot, place].astype(jnp.float32)
            done[...] = value.reshape(shape)

            @pl.when(place > 0)
            def _():
                up_copy(last, place).wait_recv()
                more = from_low[slot, place - 1].astype(jnp.float32)
                done[...] = done[...] + more.reshape(shape)

                @pl.when(last < units - DEPTH)
                def _():
                    pl.semaphore_signal(high_free, inc=1, device_id=lower, device_id_type=MESH)

            @pl.when(place < line - 1)
            def _():
                down_copy(last, place).wait_recv()
                more = from_high[slot, place].astype(jnp.float32)
                done[...] = done[...] + more.reshape(shape)

                @pl.when(last < units - DEPTH)
                def _():
                    pl.semaphore_signal(low_free, inc=1, device_id=higher, device_id_type=MESH)

            gather_terms(last)
            for copy in done_copies(last):
                copy.start()

    def unit(u, c, kind):
        slot = lax.rem(u, DEPTH)

        @pl.when(u >= DEPTH)
        def _():
            drained(u - DEPTH)

        source = lax.rem(c, kept)

        def one(j, carry):
            value = jnp.dot(mixed[source], images[2 * kind + j], preferred_element_type=jnp.float32)
            value = value.astype(jnp.bfloat16)
            for d in range(line):
                sums[slot, d, j] = value[:, d * half : (d + 1) * half]
            return carry

        lax.fori_loop(0, 2, one, 0)
        handle(u)

    def walk(start, base, kinds, fresh):
        def one(n, carry):
            c = start + n
            if fresh:
                front(c)

            def inner(k, carry):
                unit(base + n * len(kinds) + k, c, kinds[0] + k)
                return carry

            lax.fori_loop(0, len(kinds), inner, 0)
            if fresh:

                @pl.when(c + AHEAD < chunks)
                def _():
                    left(c + AHEAD)

            return carry

        return one

    for copy in beside_copies:
        copy.wait()
    lax.fori_loop(0, early, walk(0, 0, (0, 1), True), 0)
    across_copies[0].wait()
    corner_copies[0].start()
    corner_copies[0].wait()
    lax.fori_loop(0, early, walk(0, 2 * early, (2,), False), 0)
    lax.fori_loop(0, middle, walk(early, 3 * early, (0, 1, 2), True), 0)
    across_copies[1].wait()
    corner_copies[1].start()
    corner_copies[1].wait()
    lax.fori_loop(0, kept, walk(0, 3 * kept, (3,), False), 0)
    lax.fori_loop(0, chunks - kept, walk(kept, 4 * kept, (0, 1, 2, 3), True), 0)

    def finish(i, carry):
        handle(i)
        return carry

    lax.fori_loop(units, units + HOP * (line - 1), finish, 0)
    first = 0
    for index, peers in ((place, turned_line), (here, turned_blocks), (mine, [other])):
        heard[first + index] = terms[...]
        copies = [
            remote(terms, heard.at[first + index], term_send.at[first + k], term_recv.at[first + k], device)
            for k, device in enumerate(peers)
        ]
        for copy in copies:
            copy.start()
        for copy in copies:
            copy.wait()
        value = heard[first]
        for k in range(len(peers)):
            value = value + heard[first + 1 + k]
        terms[...] = value
        first += len(peers) + 1

    def whole(n):
        value = jnp.sum(terms[n], axis=1, keepdims=True)
        return jnp.sum(value, axis=0, keepdims=True) / entries

    mean_sq = whole(0)
    norm_sq = mean_sq + EPSILON
    projection = whole(1)
    alpha_coef = projection / norm_sq
    left_over = whole(2) - 2.0 * alpha_coef * projection + alpha_coef * alpha_coef * mean_sq
    beta_coef = jnp.sqrt(jnp.maximum(left_over, 0.0) / norm_sq + EPSILON)
    scale = 1.0 / (jnp.sqrt(norm_sq) * beta_coef)
    for n, value in enumerate((alpha_coef, beta_coef, scale)):
        total_ref[n] = jnp.broadcast_to(value, total_ref.shape[1:])
    for u in range(units - DEPTH, units):
        drained(u)
    for u in range(units - 2, units):
        for copy in done_copies(u):
            copy.wait()
    for c in range(chunks - AHEAD, chunks):
        for h in range(blocks):
            part_copy(c, h).wait_send()


def early_chunks(chunks):
    return 6 * chunks // 16, 3 * chunks // 16


def line_call(pair, own, left, right, line, lefts, blocks, entries):
    pairs, depth, wide = own.shape
    states = pairs // blocks
    inner = blocks * depth
    width = left.shape[0] // inner
    chunks = left.shape[1] // (lefts * STEP)
    rows = lefts * width * STEP
    lanes = right.shape[1] // line
    half = lanes // 2
    tall = states * STEP
    low = jnp.bfloat16
    hbm = pl.BlockSpec(memory_space=pltpu.MemorySpace.HBM)
    dma = pltpu.SemaphoreType.DMA
    plain = pltpu.SemaphoreType.REGULAR
    return pl.pallas_call(
        functools.partial(line_kernel, (width, blocks, states, depth, line, entries)),
        out_shape=(
            jax.ShapeDtypeStruct((blocks, states, chunks * STEP, lanes), low),
            jax.ShapeDtypeStruct((chunks, rows, inner), low),
            jax.ShapeDtypeStruct((3, 8, LANES), jnp.float32),
        ),
        in_specs=[pl.BlockSpec(memory_space=pltpu.SMEM)] + [hbm] * 3,
        out_specs=(hbm, hbm, pl.BlockSpec(memory_space=pltpu.VMEM)),
        scratch_shapes=[
            pltpu.VMEM((pairs, inner, wide), low),
            pltpu.VMEM((8, right.shape[0], line * half), low),
            pltpu.VMEM((sum(early_chunks(chunks)), tall, right.shape[0]), low),
            pltpu.VMEM((2, inner // CUT, LANES), low),
            pltpu.VMEM((2, rows, inner), low),
            pltpu.VMEM((AHEAD, 2, pairs, rows // 2, wide), low),
            pltpu.VMEM((AHEAD, pairs, rows // 2, wide), low),
            pltpu.VMEM((DEPTH, line, 2, tall, half), low),
            pltpu.VMEM((DEPTH, line - 1, 2, tall, half), low),
            pltpu.VMEM((DEPTH, line - 1, 2, tall, half), low),
            pltpu.VMEM((2, states, STEP, half), jnp.float32),
            pltpu.VMEM((2, 2, states, STEP, half), low),
            pltpu.VMEM((3, 8, LANES), jnp.float32),
            pltpu.VMEM((line + 6, 3, 8, LANES), jnp.float32),
            dma((1,)),
            dma((blocks + 1,)),
            dma((blocks + 1,)),
            dma((blocks,)),
            dma((blocks,)),
            dma((2, line)),
            dma((6,)),
            dma((6,)),
            dma((2,)),
            dma((2, LANES // STEP)),
            dma((2,)),
            dma((AHEAD, blocks)),
            dma((AHEAD, blocks)),
            plain,
            dma((DEPTH, line)),
            dma((DEPTH, line - 1)),
            dma((DEPTH, line - 1)),
            plain,
            plain,
            dma((2, 2)),
            dma((line + 6,)),
            dma((line + 6,)),
        ],
        compiler_params=pltpu.CompilerParams(
            collective_id=0, has_side_effects=True, vmem_limit_bytes=67043328
        ),
        cost_estimate=pl.CostEstimate(
            flops=2 * chunks * (rows * inner * pairs * wide + tall * right.shape[0] * 4 * line * lanes),
            bytes_accessed=4 * (left.size + own.size + right.size) + 4 * chunks * tall * blocks * lanes,
            transcendentals=0,
        ),
    )(pair.reshape(-1), own, left, right)


def lined_body(state, left_env, right_env, site_one, site_two):
    pair = pair_tensor(site_one, site_two)
    lefts, rights, owners = (lax.axis_size(name) for name in ("lb", "rb", "wa"))
    _, blocks, states, depth, lanes = state.shape
    entries = float(state.size * lefts * rights * owners)
    own = state.reshape(blocks * states, depth, lanes)
    left = left_env.reshape(-1, left_env.shape[-1])
    right = right_env.reshape(-1, right_env.shape[-1])
    applied, _, totals = line_call(pair, own, left, right, rights, lefts, blocks, entries)
    return final_call(totals, applied, state)


def final_kernel(total_ref, applied_ref, state_ref, out_ref, coef_ref):
    alpha_coef, scale = total_ref[0, 0, 0], total_ref[2, 0, 0]
    state_values = state_ref[0].astype(jnp.float32)
    out_ref[0] = (applied_ref[...].astype(jnp.float32) - alpha_coef * state_values) * scale
    for n in range(2):
        coef_ref[n] = total_ref[n, 0, 0]


def final_call(totals, applied, state):
    _, blocks, states, depth, lanes = state.shape
    smem = pl.BlockSpec(memory_space=pltpu.SMEM)
    whole = pl.BlockSpec((1, 1, 1, depth, lanes), lambda h, s: (0, h, s, 0, 0))
    return pl.pallas_call(
        final_kernel,
        grid=(blocks, states),
        out_shape=(jax.ShapeDtypeStruct(state.shape, jnp.float32), jax.ShapeDtypeStruct((2,), jnp.float32)),
        in_specs=[smem, pl.BlockSpec((1, 1, depth, lanes), lambda h, s: (h, s, 0, 0)), whole],
        out_specs=(whole, smem),
        cost_estimate=pl.CostEstimate(flops=4 * state.size, bytes_accessed=8 * state.size, transcendentals=0),
    )(totals, applied, state)


def fits(mesh):
    return (mesh.shape["lb"], mesh.shape["rb"], mesh.shape["wa"]) == (2, 4, 4)


def solution(mesh):
    placed = (
        P("wa", None, None, "lb", "rb"),
        P(None, None, "lb", "wa", None),
        P(None, None, "rb", "wa", None),
        P(),
        P(),
    )
    if fits(mesh):
        return jax.shard_map(
            lined_body,
            mesh=mesh,
            in_specs=placed,
            out_specs=(P("wa", None, None, "lb", "rb"), P()),
            check_vma=False,
        )
    return jax.shard_map(
        body,
        mesh=mesh,
        in_specs=placed,
        out_specs=(P("wa", None, None, "lb", "rb"), P()),
        check_vma=False,
    )
```

```python
import functools
import jax
import jax.numpy as jnp
from jax import lax
from jax.experimental import pallas as pl
from jax.experimental.pallas import tpu as pltpu
from jax.sharding import PartitionSpec as P

EPSILON = 1e-06
CHUNKS = 4
GATHERS = 2


def pair_tensor(site_one, site_two):
    joined = jnp.einsum("wuac,uvbd->wvabcd", site_one, site_two, precision=lax.Precision.HIGHEST)
    mpo_width = site_one.shape[0]
    states = site_one.shape[2] * site_two.shape[2]
    return joined.reshape(mpo_width, mpo_width, states, states)


def mix_kernel(terms, pair_ref, *refs):
    out_ref = refs[terms]
    width, _, states, rows, _ = refs[0].shape
    step = 16

    @pl.loop(0, rows // step)
    def _(block):
        span = pl.ds(pl.multiple_of(block * step, step), step)
        planes = []
        for w in range(width):
            for s in range(states):
                value = refs[0][w, 0, s, span, :].astype(jnp.float32)
                for other in refs[1:terms]:
                    value = value + other[w, 0, s, span, :].astype(jnp.float32)
                planes.append(value)
        for v in range(width):
            for t in range(states):
                total = None
                for w in range(width):
                    for s in range(states):
                        entry = pair_ref[((w * width + v) * states + s) * states + t]
                        term = planes[w * states + s] * entry
                        total = term if total is None else total + term
                out_ref[v, 0, t, span, :] = total.astype(out_ref.dtype)


def mix(pair, parts):
    width, blocks, states, rows, lanes = parts[0].shape
    spec = pl.BlockSpec((width, 1, states, rows, lanes), lambda h: (0, h, 0, 0, 0))
    count = width * states
    size = parts[0].size
    return pl.pallas_call(
        functools.partial(mix_kernel, len(parts)),
        grid=(blocks,),
        out_shape=jax.ShapeDtypeStruct(parts[0].shape, jnp.bfloat16),
        in_specs=[pl.BlockSpec(memory_space=pltpu.SMEM)] + [spec] * len(parts),
        out_specs=spec,
        cost_estimate=pl.CostEstimate(
            flops=2 * size * count * 16, bytes_accessed=2 * size * (len(parts) + 1), transcendentals=0
        ),
    )(pair.reshape(-1), *parts)


def body(state, left_env, right_env, site_one, site_two):
    pair = pair_tensor(site_one, site_two)
    lefts, rights, owners = (lax.axis_size(name) for name in ("lb", "rb", "wa"))
    mine = lax.axis_index("lb")
    here = lax.axis_index("wa")
    _, blocks, _, _, _ = state.shape
    entries = float(state.size * lefts * rights * owners)

    group = blocks // GATHERS
    gathered = []
    for h in range(0, blocks, group):
        gathered.append(lax.all_gather(state[:, h : h + group], "wa", axis=0, tiled=True))
    turned = jnp.transpose(left_env[:, :, :, 0, :], (0, 1, 3, 2))
    owned = turned.shape[2] // lefts
    chunk = owned // CHUNKS

    def left_part(owner, position):
        rows = lax.dynamic_slice_in_dim(turned, owner * owned + position * chunk, chunk, 2)
        return [
            jnp.einsum(
                "wgpm,ghsmn->whspn", rows, part, preferred_element_type=jnp.float32
            ).astype(jnp.bfloat16)
            for part in gathered
        ]

    envs = {0: right_env[:, :, :, 0, :]}
    bit = owners // 2
    while bit:
        swap = [(a, a ^ bit) for a in range(owners)]
        for r in list(envs):
            envs[r ^ bit] = lax.ppermute(envs[r], "wa", swap)
        bit //= 2
    order = sorted(envs)
    near, far = order[: owners // 2], order[owners // 2 :]
    width, wide = envs[0].shape[0], envs[0].shape[3]

    def joined(pack):
        env = jnp.concatenate([envs[r] for r in pack], axis=3)
        return env.reshape(width, blocks, -1, len(pack), wide)

    packs = [(pack, joined(pack)) for pack in (near, far, order)]

    images = {r: [] for r in order}
    for position in range(CHUNKS):
        arrived = []
        for shift in range(1, lefts):
            sent = left_part(lax.rem(mine + shift, lefts), position)
            ring = [(a, (a + shift) % lefts) for a in range(lefts)]
            arrived.append([lax.ppermute(piece, "lb", ring) for piece in sent])
        parts = [jnp.concatenate(p, axis=1) for p in [left_part(mine, position)] + arrived]
        mixed = mix(pair, parts)
        for pack, env in packs[:2] if position == 0 else packs[2:]:
            part = jnp.einsum("vhtpn,vhndq->dtpq", mixed, env, preferred_element_type=jnp.float32).astype(jnp.bfloat16)
            part = lax.psum_scatter(part, "rb", scatter_dimension=3, tiled=True)
            for r, piece in zip(pack, part):
                images[r].append(piece)
    applied = [jnp.concatenate(images[r], axis=1).astype(jnp.float32) for r in order]
    vectors = [
        lax.dynamic_index_in_dim(state[0], here ^ r, 0, keepdims=False).astype(jnp.float32)
        for r in order
    ]
    state_values = state.astype(jnp.float32)
    terms = jnp.stack(
        [
            jnp.sum(state_values * state_values),
            sum(jnp.sum(s * a) for s, a in zip(vectors, applied)),
            sum(jnp.sum(a * a) for a in applied),
        ]
    )
    for name in ("wa", "lb", "rb"):
        size, bit = lax.axis_size(name), 1
        while bit < size:
            terms = terms + lax.ppermute(terms, name, [(a, a ^ bit) for a in range(size)])
            bit *= 2
    squares, crossed, image_squares = terms
    norm_sq = squares / entries + EPSILON
    projection = crossed / entries
    alpha_coef = projection / norm_sq
    beta_coef = jnp.sqrt((image_squares / entries - alpha_coef * projection) / norm_sq + EPSILON)
    scale = 1.0 / (jnp.sqrt(norm_sq) * beta_coef)
    result = jnp.zeros(state.shape, jnp.float32)
    for r, s, a in zip(order, vectors, applied):
        value = (a - alpha_coef * s) * scale
        result = lax.dynamic_update_slice(result, value[None, None], (0, here ^ r, 0, 0, 0))
    return (result, jnp.stack([alpha_coef, beta_coef]))


MESH = pl.DeviceIdType.MESH
STEP = 32
DEPTH = 8
HOP = 2
AHEAD = 4
CUT = 2
PART = 2
PIECES = 4
LANES = 128


def line_kernel(
    sizes,
    pair_ref,
    own_ref,
    left_ref,
    right_ref,
    out_ref,
    env_ref,
    total_ref,
    psi,
    images,
    mixed,
    rows_buf,
    parts,
    arrived,
    sums,
    from_low,
    from_high,
    done,
    ready,
    terms,
    heard,
    load_sem,
    psi_send,
    psi_recv,
    relay_send,
    relay_recv,
    right_load,
    right_send,
    right_recv,
    raw_sem,
    turn_sem,
    rows_sem,
    part_send,
    part_recv,
    part_free,
    sum_send,
    low_recv,
    high_recv,
    low_free,
    high_free,
    done_sem,
    term_send,
    term_recv,
):
    width, blocks, states, depth, line, entries = sizes
    chunks = env_ref.shape[0]
    units = 4 * chunks
    early, middle = early_chunks(chunks)
    kept = early + middle
    groups = blocks * states // PART
    inner = blocks * depth
    piece = inner // CUT
    mine = lax.axis_index("lb")
    place = lax.axis_index("rb")
    here = lax.axis_index("wa")
    beside = here + 1 - 2 * lax.rem(here, 2)
    across = lax.rem(here + 2, 4)
    corner = 3 - here
    partner = (mine, place, beside)
    opposite = (mine, place, across)
    other = (1 - mine, place, here)
    higher = (mine, lax.rem(place + 1, line), here)
    lower = (mine, lax.rem(place + line - 1, line), here)
    turned_line = [(mine, lax.rem(place + k, line), here) for k in range(1, line)]
    turned_blocks = [(mine, place, lax.rem(here + k, 4)) for k in range(1, 4)]

    def remote(source, target, send, recv, device):
        return pltpu.make_async_remote_copy(
            src_ref=source, dst_ref=target, send_sem=send, recv_sem=recv, device_id=device, device_id_type=MESH
        )

    my_span = pl.ds(pl.multiple_of(here * depth, depth), depth)
    across_span = pl.ds(pl.multiple_of(across * depth, depth), depth)
    own_copy = pltpu.make_async_copy(own_ref, psi.at[:, my_span, :], load_sem.at[0])
    own_copy.start()

    tiles = piece // LANES

    def raw_copies(n):
        slot = lax.rem(n, 2)
        q = n // (2 * width * CUT)
        side = lax.rem(n // (width * CUT), 2)
        row = lax.rem(n, width * CUT) * piece
        first = side * (chunks * STEP) + q * LANES
        return [
            pltpu.make_async_copy(
                left_ref.at[
                    pl.ds(pl.multiple_of(row + k * LANES, LANES), LANES), pl.ds(pl.multiple_of(first, LANES), LANES)
                ],
                mixed.at[2 + slot, :, pl.ds(k * LANES, LANES)],
                raw_sem.at[slot, k],
            )
            for k in range(tiles)
        ]

    for copy in raw_copies(0):
        copy.start()

    barrier = pltpu.get_barrier_semaphore()
    devices = turned_line + turned_blocks + [other]
    for device in devices:
        pl.semaphore_signal(barrier, inc=1, device_id=device, device_id_type=MESH)
    pl.semaphore_wait(barrier, len(devices))

    def group(g):
        return pl.ds(g * PART, PART)

    psi_copies = [
        remote(own_ref.at[group(g)], psi.at[group(g), my_span, :], psi_send.at[g], psi_recv.at[g], opposite)
        for g in range(groups)
    ]
    for copy in psi_copies:
        copy.start()
    share = remote(own_ref, psi.at[:, my_span, :], psi_send.at[groups], psi_recv.at[groups], partner)
    share.start()

    lanes = right_ref.shape[1] // line
    half = lanes // 2
    local = []
    for part in range(2):
        for d in range(line):
            local.append(
                pltpu.make_async_copy(
                    right_ref.at[:, pl.ds(d * lanes + part * half, half)],
                    images.at[part, :, pl.ds(d * half, half)],
                    right_load.at[part, d],
                )
            )
    for copy in local:
        copy.start()

    turns = 2 * width * CUT * chunks * STEP // LANES
    cuts = LANES // STEP

    def turned_copies(n):
        slot = lax.rem(n, 2)
        q = n // (2 * width * CUT)
        side = lax.rem(n // (width * CUT), 2)
        w = lax.rem(n // CUT, width)
        first = (side * width + w) * STEP
        column = pl.multiple_of(lax.rem(n, CUT) * piece, piece)
        return [
            pltpu.make_async_copy(
                mixed.at[slot, pl.ds(k * STEP, STEP), pl.ds(0, piece)],
                env_ref.at[q * cuts + k, pl.ds(pl.multiple_of(first, STEP), STEP), pl.ds(column, piece)],
                turn_sem.at[slot, k],
            )
            for k in range(cuts)
        ]

    def turn(n, carry):
        slot = lax.rem(n, 2)

        @pl.when(n + 1 < turns)
        def _():
            for copy in raw_copies(n + 1):
                copy.start()

        for copy in raw_copies(n):
            copy.wait()

        @pl.when(n >= 2)
        def _():
            for copy in turned_copies(n - 2):
                copy.wait()

        for k in range(tiles):
            span = pl.ds(k * LANES, LANES)
            mixed[slot, :, span] = mixed[2 + slot, :, span].T
        for copy in turned_copies(n):
            copy.start()
        return carry

    lax.fori_loop(0, turns, turn, 0)
    for n in range(turns - 2, turns):
        for copy in turned_copies(n):
            copy.wait()

    def rows_copy(n, c):
        slot = lax.rem(n, 2)
        return pltpu.make_async_copy(env_ref.at[c], rows_buf.at[slot], rows_sem.at[slot])

    rows_copy(0, 0).start()
    own_copy.wait()
    terms[...] = jnp.zeros_like(terms)

    def folded(value):
        return jnp.sum(value.reshape(-1, 8, LANES), axis=0)

    def square(p, carry):
        value = psi[p, my_span, :].astype(jnp.float32)
        value = value * value
        for n in range(value.shape[1] // LANES):
            terms[0] += folded(value[:, n * LANES : (n + 1) * LANES])
        return carry

    lax.fori_loop(0, blocks * states, square, 0)
    for copy in local:
        copy.wait()

    def image_copy(n, source, target, device):
        return remote(images.at[source], images.at[target], right_send.at[n], right_recv.at[n], device)

    tall = images.shape[1] // PIECES

    def piece_copy(n, source, target, k, device):
        span = pl.ds(k * tall, tall)
        return remote(
            images.at[source, span], images.at[target, span], right_send.at[n + k], right_recv.at[n + k], device
        )

    beside_copies = [image_copy(0, 0, 2, partner), image_copy(1, 1, 3, partner)]
    across_copies, corner_copies = [], []
    for part in range(2):
        n = 2 + 2 * part * PIECES
        target = 4 + 2 * part
        across_copies.append([piece_copy(n, part, target, k, opposite) for k in range(PIECES)])
        corner_copies.append([piece_copy(n + PIECES, target, target + 1, k, partner) for k in range(PIECES)])

    def settle(part):
        for first, second in zip(across_copies[part], corner_copies[part]):
            first.wait()
            second.start()
        for copy in corner_copies[part]:
            copy.wait()

    def part_copy(c, g):
        slot = lax.rem(c, AHEAD)
        return remote(
            parts.at[slot, 1 - mine, group(g)],
            arrived.at[slot, group(g)],
            part_send.at[slot, g],
            part_recv.at[slot, g],
            other,
        )

    def left_block(c, n, g):
        slot = lax.rem(c, AHEAD)
        source = lax.rem(n, 2)

        def one(s, carry):
            p = g * PART + s
            value = jnp.dot(rows_buf[source], psi[p], preferred_element_type=jnp.float32)
            value = value.astype(jnp.bfloat16)
            rows = value.shape[0] // 2
            parts[slot, 0, p] = value[:rows]
            parts[slot, 1, p] = value[rows:]
            return carry

        lax.fori_loop(0, PART, one, 0)
        part_copy(c, g).start()

    share.wait()
    for g in range(groups):
        psi_copies[g].wait()
        if g == groups - 1:
            for copy in across_copies[0] + across_copies[1]:
                copy.start()
        relay = remote(
            psi.at[group(g), across_span, :], psi.at[group(g), across_span, :], relay_send.at[g], relay_recv.at[g], partner
        )
        relay.start()
        if g == 0:
            for copy in beside_copies:
                copy.start()
        relay.wait()

        def one(c, carry):
            n = g * AHEAD + c
            rows_copy(n, c).wait()
            rows_copy(n + 1, jnp.where(n == groups * AHEAD - 1, AHEAD, lax.rem(c + 1, AHEAD))).start()
            left_block(c, n, g)
            return carry

        lax.fori_loop(0, AHEAD, one, 0)

    def left(c):
        n = c + (groups - 1) * AHEAD
        for g in range(groups):
            part_copy(c - AHEAD, g).wait_send()

        pl.semaphore_wait(part_free, 1)

        rows_copy(n, c).wait()

        @pl.when(c + 1 < chunks)
        def _():
            rows_copy(n + 1, c + 1).start()

        def one(g, carry):
            left_block(c, n, g)
            return carry

        lax.fori_loop(0, groups, one, 0)

    def front(c):
        slot = lax.rem(c, AHEAD)
        source = lax.rem(c, AHEAD)
        target = lax.rem(c, kept)
        tile = 16
        wide = psi.shape[2]

        def one(h, carry):
            for k in range(states // PART):
                part_copy(c, h * (states // PART) + k).wait_recv()
            for step in range(STEP // tile):
                planes = []
                for w in range(width):
                    for s in range(states):
                        span = pl.ds(w * STEP + step * tile, tile)
                        value = parts[slot, mine, h * states + s, span, :].astype(jnp.float32)
                        value = value + arrived[source, h * states + s, span, :].astype(jnp.float32)
                        planes.append(value)
                for v in range(width):
                    for t in range(states):
                        total = None
                        for w in range(width):
                            for s in range(states):
                                entry = pair_ref[((w * width + v) * states + s) * states + t]
                                term = planes[w * states + s] * entry
                                total = term if total is None else total + term
                        column = pl.multiple_of((v * blocks + h) * wide, wide)
                        mixed[target, pl.ds(t * STEP + step * tile, tile), pl.ds(column, wide)] = total.astype(
                            jnp.bfloat16
                        )
            return carry

        lax.fori_loop(0, blocks, one, 0)

        @pl.when(c + AHEAD < chunks)
        def _():
            pl.semaphore_signal(part_free, inc=1, device_id=other, device_id_type=MESH)

    def up_copy(u, d):
        slot = lax.rem(u, DEPTH)
        return remote(sums.at[slot, d], from_low.at[slot, d - 1], sum_send.at[slot, d], low_recv.at[slot, d - 1], higher)

    def down_copy(u, d):
        slot = lax.rem(u, DEPTH)
        return remote(sums.at[slot, d], from_high.at[slot, d], sum_send.at[slot, d], high_recv.at[slot, d], lower)

    def drained(u):
        for d in range(line):

            @pl.when(d > place)
            def _():
                up_copy(u, d).wait_send()

            @pl.when(d < place)
            def _():
                down_copy(u, d).wait_send()

    def added(slot, d, source, n):
        total = sums[slot, d].astype(jnp.float32) + source[slot, n].astype(jnp.float32)
        sums[slot, d] = total.astype(jnp.bfloat16)

    def where_to(u):
        second, third, fourth = 3 * early, 3 * early + 3 * middle, 4 * (early + middle)
        e, f = lax.rem(u + 3 * units - second, 3), lax.rem(u + 4 * units - fourth, 4)
        chunk = jnp.where(u < fourth, u - third, kept + (u - fourth) // 4)
        chunk = jnp.where(u < third, early + (u - second) // 3, chunk)
        chunk = jnp.where(u < second, u - 2 * early, chunk)
        chunk = jnp.where(u < 2 * early, u // 2, chunk)
        kind = jnp.where(u < fourth, 3, f)
        kind = jnp.where(u < third, e, kind)
        kind = jnp.where(u < second, 2, kind)
        kind = jnp.where(u < 2 * early, lax.rem(u, 2), kind)
        return chunk, kind

    def places(u):
        chunk, kind = where_to(u)
        far = kind // 2
        near_block = here + kind * (beside - here)
        spots = []
        for j in range(2):
            far_block = corner if j else across
            block = (1 - far) * near_block + far * far_block
            column = (1 - far) * j + far * (kind - 2)
            spots.append((block, column))
        return chunk, spots

    def done_copies(u):
        chunk, spots = places(u)
        copies = []
        for j, (block, column) in enumerate(spots):
            copies.append(
                pltpu.make_async_copy(
                    ready.at[j],
                    out_ref.at[
                        block,
                        :,
                        pl.ds(pl.multiple_of(chunk * STEP, STEP), STEP),
                        pl.ds(pl.multiple_of(column * half, half), half),
                    ],
                    done_sem.at[j],
                )
            )
        return copies

    def gather_terms(u):
        chunk, spots = places(u)
        first = pl.multiple_of(here * depth + chunk * STEP, STEP)
        for j, (block, column) in enumerate(spots):
            for t in range(states):
                value = done[j, t]
                ready[j, t] = value.astype(ready.dtype)
                start = psi[block * states + t, pl.ds(first, STEP), pl.ds(pl.multiple_of(column * half, half), half)]
                start = start.astype(jnp.float32)
                terms[1] += folded(start * value)
                terms[2] += folded(value * value)

    def handle(i):
        up = i - HOP * place
        slot_up = lax.rem(up + DEPTH * HOP * line, DEPTH)

        @pl.when(jnp.logical_and(place < line - 1, jnp.logical_and(up >= 0, up < units)))
        def _():
            @pl.when(up >= DEPTH)
            def _():
                pl.semaphore_wait(high_free, 1)

            for d in range(line - 1, 0, -1):

                @pl.when(d > place)
                def _():
                    @pl.when(place > 0)
                    def _():
                        up_copy(up, d).wait_recv()
                        added(slot_up, d, from_low, d - 1)

                    up_copy(up, d).start()

        down = i - HOP * (line - 1 - place)
        slot_down = lax.rem(down + DEPTH * HOP * line, DEPTH)

        @pl.when(jnp.logical_and(place > 0, jnp.logical_and(down >= 0, down < units)))
        def _():
            @pl.when(down >= DEPTH)
            def _():
                pl.semaphore_wait(low_free, 1)

            for d in range(line - 1):

                @pl.when(d < place)
                def _():
                    @pl.when(place < line - 1)
                    def _():
                        down_copy(down, d).wait_recv()
                        added(slot_down, d, from_high, d)

                    down_copy(down, d).start()

        last = i - HOP * (line - 1)

        @pl.when(last >= 0)
        def _():
            slot = lax.rem(last, DEPTH)

            @pl.when(last >= 1)
            def _():
                for copy in done_copies(last - 1):
                    copy.wait()

            shape = done.shape
            value = sums[slot, place].astype(jnp.float32)
            done[...] = value.reshape(shape)

            @pl.when(place > 0)
            def _():
                up_copy(last, place).wait_recv()
                more = from_low[slot, place - 1].astype(jnp.float32)
                done[...] = done[...] + more.reshape(shape)

                @pl.when(last < units - DEPTH)
                def _():
                    pl.semaphore_signal(high_free, inc=1, device_id=lower, device_id_type=MESH)

            @pl.when(place < line - 1)
            def _():
                down_copy(last, place).wait_recv()
                more = from_high[slot, place].astype(jnp.float32)
                done[...] = done[...] + more.reshape(shape)

                @pl.when(last < units - DEPTH)
                def _():
                    pl.semaphore_signal(low_free, inc=1, device_id=higher, device_id_type=MESH)

            gather_terms(last)
            for copy in done_copies(last):
                copy.start()

    def unit(u, c, kind):
        slot = lax.rem(u, DEPTH)

        @pl.when(u >= DEPTH)
        def _():
            drained(u - DEPTH)

        source = lax.rem(c, kept)

        def one(j, carry):
            value = jnp.dot(mixed[source], images[2 * kind + j], preferred_element_type=jnp.float32)
            value = value.astype(jnp.bfloat16)
            for d in range(line):
                sums[slot, d, j] = value[:, d * half : (d + 1) * half]
            return carry

        lax.fori_loop(0, 2, one, 0)
        handle(u)

    def walk(start, base, kinds, fresh):
        def one(n, carry):
            c = start + n
            if fresh:
                front(c)

            def inner(k, carry):
                unit(base + n * len(kinds) + k, c, kinds[0] + k)
                return carry

            lax.fori_loop(0, len(kinds), inner, 0)
            if fresh:

                @pl.when(c + AHEAD < chunks)
                def _():
                    left(c + AHEAD)

            return carry

        return one

    for copy in beside_copies:
        copy.wait()
    lax.fori_loop(0, early, walk(0, 0, (0, 1), True), 0)
    settle(0)
    lax.fori_loop(0, early, walk(0, 2 * early, (2,), False), 0)
    lax.fori_loop(0, middle, walk(early, 3 * early, (0, 1, 2), True), 0)
    settle(1)
    lax.fori_loop(0, kept, walk(0, 3 * kept, (3,), False), 0)
    lax.fori_loop(0, chunks - kept, walk(kept, 4 * kept, (0, 1, 2, 3), True), 0)

    def finish(i, carry):
        handle(i)
        return carry

    lax.fori_loop(units, units + HOP * (line - 1), finish, 0)
    first = 0
    for index, peers in ((place, turned_line), (here, turned_blocks), (mine, [other])):
        heard[first + index] = terms[...]
        copies = [
            remote(terms, heard.at[first + index], term_send.at[first + k], term_recv.at[first + k], device)
            for k, device in enumerate(peers)
        ]
        for copy in copies:
            copy.start()
        for copy in copies:
            copy.wait()
        value = heard[first]
        for k in range(len(peers)):
            value = value + heard[first + 1 + k]
        terms[...] = value
        first += len(peers) + 1

    def whole(n):
        value = jnp.sum(terms[n], axis=1, keepdims=True)
        return jnp.sum(value, axis=0, keepdims=True) / entries

    mean_sq = whole(0)
    norm_sq = mean_sq + EPSILON
    projection = whole(1)
    alpha_coef = projection / norm_sq
    left_over = whole(2) - 2.0 * alpha_coef * projection + alpha_coef * alpha_coef * mean_sq
    beta_coef = jnp.sqrt(jnp.maximum(left_over, 0.0) / norm_sq + EPSILON)
    scale = 1.0 / (jnp.sqrt(norm_sq) * beta_coef)
    for n, value in enumerate((alpha_coef, beta_coef, scale)):
        total_ref[n] = jnp.broadcast_to(value, total_ref.shape[1:])
    for u in range(units - DEPTH, units):
        drained(u)
    for copy in done_copies(units - 1):
        copy.wait()
    for c in range(chunks - AHEAD, chunks):
        for g in range(groups):
            part_copy(c, g).wait_send()


def early_chunks(chunks):
    return 6 * chunks // 16, 4 * chunks // 16


def line_call(pair, own, left, right, line, lefts, blocks, entries):
    pairs, depth, wide = own.shape
    states = pairs // blocks
    inner = blocks * depth
    width = left.shape[0] // inner
    chunks = left.shape[1] // (lefts * STEP)
    rows = lefts * width * STEP
    groups = pairs // PART
    lanes = right.shape[1] // line
    half = lanes // 2
    tall = states * STEP
    low = jnp.bfloat16
    hbm = pl.BlockSpec(memory_space=pltpu.MemorySpace.HBM)
    dma = pltpu.SemaphoreType.DMA
    plain = pltpu.SemaphoreType.REGULAR
    return pl.pallas_call(
        functools.partial(line_kernel, (width, blocks, states, depth, line, entries)),
        out_shape=(
            jax.ShapeDtypeStruct((blocks, states, chunks * STEP, lanes), low),
            jax.ShapeDtypeStruct((chunks, rows, inner), low),
            jax.ShapeDtypeStruct((3, 8, LANES), jnp.float32),
        ),
        in_specs=[pl.BlockSpec(memory_space=pltpu.SMEM)] + [hbm] * 3,
        out_specs=(hbm, hbm, pl.BlockSpec(memory_space=pltpu.VMEM)),
        scratch_shapes=[
            pltpu.VMEM((pairs, inner, wide), low),
            pltpu.VMEM((8, right.shape[0], line * half), low),
            pltpu.VMEM((sum(early_chunks(chunks)), tall, right.shape[0]), low),
            pltpu.VMEM((2, rows, inner), low),
            pltpu.VMEM((AHEAD, 2, pairs, rows // 2, wide), low),
            pltpu.VMEM((AHEAD, pairs, rows // 2, wide), low),
            pltpu.VMEM((DEPTH, line, 2, tall, half), low),
            pltpu.VMEM((DEPTH, line - 1, 2, tall, half), low),
            pltpu.VMEM((DEPTH, line - 1, 2, tall, half), low),
            pltpu.VMEM((2, states, STEP, half), jnp.float32),
            pltpu.VMEM((2, states, STEP, half), low),
            pltpu.VMEM((3, 8, LANES), jnp.float32),
            pltpu.VMEM((line + 6, 3, 8, LANES), jnp.float32),
            dma((1,)),
            dma((groups + 1,)),
            dma((groups + 1,)),
            dma((groups,)),
            dma((groups,)),
            dma((2, line)),
            dma((2 + 4 * PIECES,)),
            dma((2 + 4 * PIECES,)),
            dma((2, inner // CUT // LANES)),
            dma((2, LANES // STEP)),
            dma((2,)),
            dma((AHEAD, groups)),
            dma((AHEAD, groups)),
            plain,
            dma((DEPTH, line)),
            dma((DEPTH, line - 1)),
            dma((DEPTH, line - 1)),
            plain,
            plain,
            dma((2,)),
            dma((line + 6,)),
            dma((line + 6,)),
        ],
        compiler_params=pltpu.CompilerParams(
            collective_id=0, has_side_effects=True, vmem_limit_bytes=67043328
        ),
        cost_estimate=pl.CostEstimate(
            flops=2 * chunks * (rows * inner * pairs * wide + tall * right.shape[0] * 4 * line * lanes),
            bytes_accessed=4 * (left.size + own.size + right.size) + 4 * chunks * tall * blocks * lanes,
            transcendentals=0,
        ),
    )(pair.reshape(-1), own, left, right)


def lined_body(state, left_env, right_env, site_one, site_two):
    pair = pair_tensor(site_one, site_two)
    lefts, rights, owners = (lax.axis_size(name) for name in ("lb", "rb", "wa"))
    _, blocks, states, depth, lanes = state.shape
    entries = float(state.size * lefts * rights * owners)
    own = state.reshape(blocks * states, depth, lanes)
    left = left_env.reshape(-1, left_env.shape[-1])
    right = right_env.reshape(-1, right_env.shape[-1])
    applied, _, totals = line_call(pair, own, left, right, rights, lefts, blocks, entries)
    return final_call(totals, applied, state)


def final_kernel(total_ref, applied_ref, state_ref, out_ref, coef_ref):
    alpha_coef, scale = total_ref[0, 0, 0], total_ref[2, 0, 0]
    state_values = state_ref[0].astype(jnp.float32)
    out_ref[0] = (applied_ref[...].astype(jnp.float32) - alpha_coef * state_values) * scale
    for n in range(2):
        coef_ref[n] = total_ref[n, 0, 0]


def final_call(totals, applied, state):
    _, blocks, states, depth, lanes = state.shape
    smem = pl.BlockSpec(memory_space=pltpu.SMEM)
    whole = pl.BlockSpec((1, 1, states, depth, lanes), lambda h: (0, h, 0, 0, 0))
    return pl.pallas_call(
        final_kernel,
        grid=(blocks,),
        out_shape=(jax.ShapeDtypeStruct(state.shape, jnp.float32), jax.ShapeDtypeStruct((2,), jnp.float32)),
        in_specs=[smem, pl.BlockSpec((1, states, depth, lanes), lambda h: (h, 0, 0, 0)), whole],
        out_specs=(whole, smem),
        cost_estimate=pl.CostEstimate(flops=4 * state.size, bytes_accessed=8 * state.size, transcendentals=0),
    )(totals, applied, state)


def fits(mesh):
    return (mesh.shape["lb"], mesh.shape["rb"], mesh.shape["wa"]) == (2, 4, 4)


def solution(mesh):
    placed = (
        P("wa", None, None, "lb", "rb"),
        P(None, None, "lb", "wa", None),
        P(None, None, "rb", "wa", None),
        P(),
        P(),
    )
    if fits(mesh):
        return jax.shard_map(
            lined_body,
            mesh=mesh,
            in_specs=placed,
            out_specs=(P("wa", None, None, "lb", "rb"), P()),
            check_vma=False,
        )
    return jax.shard_map(
        body,
        mesh=mesh,
        in_specs=placed,
        out_specs=(P("wa", None, None, "lb", "rb"), P()),
        check_vma=False,
    )
```
